32 devices in a mesh: dev: 32 (over z, y, x, core).
Axes of the slice: x: 2, y: 2, z: 4, core: 2. Of those that a mesh axis runs over, the one named last changes fastest.
Arguments:
- dual_blocks: bfloat16 [32, 3072, 3072], P('dev'), as said below
- rigid_modes: float32 [32, 6, 3072], P('dev'), may hold values from -5 to 5
- dual_local: float32 [32, 8, 3072], P('dev'), may hold values from -6 to 6
- coarse_rhs: float32 [32, 6, 8], P('dev'), may hold values from -4608 to 4608
- iface_sizes: int32 [32], P('dev'), may hold values from 1536 to 3072, as said below
- neighbours: int32 [32, 6], P('dev'), may hold values from -1 to 31, as said below
- shared_counts: int32 [32, 6], P('dev'), may hold values from 256 to 512, as said below
- iface_map: int32 [32, 3072], P('dev'), may hold values from -1 to 3071, as said below
- owner: int32 [32], replicated, may hold values from 0 to 31, as said below
Outputs:
- multipliers: float32 [32, 8, 3072], P('dev')
- projected_residual: float32 [32, 8, 3072], P('dev')
The draws below stay inside these ranges and needn't reach their ends.
Inputs may be any that keep to these rules, and one draw needn't show every extreme that they name: `dual_blocks`: each block is symmetric positive definite, and so is each of its leading principal parts. Grid subdomain g is held by slot owner[g] = (g + s) mod 32 for one offset s of the draw, so the subdomains across the faces -x, +x, -y, +y, -z, +z of slot i sit in slots i - 1, i + 1, i - 4, i + 4, i - 16, i + 16, taken mod 32. `neighbours`: the subdomains form a grid of 4 x 4 x 32/16 with g = x + 4 y + 16 z. Row i lists, for the faces -x, +x, -y, +y, -z, +z of the subdomain held in slot i, the grid subdomain across that face, or -1 on the outer boundary; across a face from g the opposite face names g. `shared_counts`: equal on both sides of a shared face; some subdomain has 512 on all its faces. `iface_sizes`: the sum of the slot's shared_counts row; some subdomain has 3072. `iface_map`: for j < iface_sizes[i], entry j is f * 512 + p for the dof at position p of face f of slot i (p below that face's count), each such code once; -1 beyond. The dof at position p of a shared face pairs with the dof at position p of the opposite face of the neighbour.
All inputs are finite; a program needn't handle non-finite values.
Results may differ from the reference program's by a relative error of at most 0.025.
Values sent between devices are 32-bit elements; how exact they have to be, the bound alone decides.
A program may use at most 128 MiB of HBM per device.

```python
import math
import jax
import jax.numpy as jnp
from jax import lax

FACES = 6
MODES = 6
CAP = 512
NMAX = 3072
LOADS = 8
ITERS = 3
NSUB = 32


def grid_links():
    layers = NSUB // 16
    identity = jnp.arange(NSUB, dtype=jnp.int32)
    along_x = identity % 4
    along_y = identity // 4 % 4
    along_z = identity // 16
    columns = [jnp.where(along_x > 0, identity - 1, -1), jnp.where(along_x < 3, identity + 1, -1), jnp.where(along_y > 0, identity - 4, -1), jnp.where(along_y < 3, identity + 4, -1), jnp.where(along_z > 0, identity - 16, -1), jnp.where(along_z < layers - 1, identity + 16, -1)]
    return jnp.stack(columns, axis=1).astype(jnp.int32)


def layout_draw(key):
    base = jax.random.fold_in(key, 7301)
    key_count, key_star, key_owner, key_order = jax.random.split(base, 4)
    links = grid_links()
    drawn = jax.random.randint(key_count, (NSUB, FACES), CAP // 2, CAP + 1, dtype=jnp.int32)
    star = jax.random.randint(key_star, (), 0, NSUB, dtype=jnp.int32)
    drawn = drawn.at[star].set(CAP)
    for lower_face in (0, 2, 4):
        across = links[star, lower_face]
        drawn = drawn.at[jnp.where(across < 0, star, across), lower_face + 1].set(CAP)
    counts = drawn
    for lower_face in (0, 2, 4):
        across = links[:, lower_face]
        mirrored = drawn[jnp.clip(across, 0, NSUB - 1), lower_face + 1]
        counts = counts.at[:, lower_face].set(jnp.where(across < 0, drawn[:, lower_face], mirrored))
    offset = jax.random.randint(key_owner, (), 1, NSUB, dtype=jnp.int32)
    identity = jnp.arange(NSUB, dtype=jnp.int32)
    owner = ((identity + offset) % NSUB).astype(jnp.int32)
    hosted = ((identity - offset + NSUB) % NSUB).astype(jnp.int32)
    slot_links = links[hosted]
    slot_counts = counts[hosted]
    sizes = jnp.sum(slot_counts, axis=1).astype(jnp.int32)
    codes_all = jnp.arange(FACES * CAP, dtype=jnp.int32)
    live_codes = (codes_all % CAP)[None, :] < slot_counts[:, codes_all // CAP]
    slot_keys = jax.random.split(key_order, NSUB)
    shuffles = jax.vmap(lambda slot_key: jax.random.permutation(slot_key, FACES * CAP))(slot_keys).astype(jnp.int32)
    scores = shuffles + jnp.where(live_codes, 0, FACES * CAP).astype(jnp.int32)
    ordered = jnp.argsort(scores, axis=1, stable=True).astype(jnp.int32)
    positions = jnp.arange(NMAX, dtype=jnp.int32)
    iface_map = jnp.where(positions[None, :] < sizes[:, None], ordered, -1).astype(jnp.int32)
    return (owner, sizes, slot_links, slot_counts, iface_map, hosted)


def draw_owner(key, part):
    return layout_draw(key)[0]


def draw_iface_sizes(key, part):
    return layout_draw(key)[1]


def draw_neighbours(key, part):
    return layout_draw(key)[2]


def draw_shared_counts(key, part):
    return layout_draw(key)[3]


def draw_iface_map(key, part):
    return layout_draw(key)[4]


def mode_sample(sample_key, shape):
    values = jnp.clip(jax.random.normal(sample_key, shape, jnp.float32), -4.0, 4.0)
    return values


def draw_rigid_modes(key, part):
    owner, sizes, slot_links, slot_counts, iface_map, hosted = layout_draw(key)
    base = jax.random.fold_in(key, 7303)
    key_common, key_edge, key_own = jax.random.split(base, 3)
    common = mode_sample(key_common, (NSUB, 3, MODES, CAP))
    edge = mode_sample(key_edge, (NSUB, FACES, MODES, CAP))
    own = mode_sample(key_own, (NSUB, MODES, NMAX))
    face_ids = jnp.arange(FACES, dtype=jnp.int32)
    upper = face_ids % 2 == 1
    face_key = jnp.where(upper[None, :], hosted[:, None], slot_links)
    face_key = jnp.clip(face_key, 0, NSUB - 1).astype(jnp.int32)
    axis_ids = (face_ids // 2).astype(jnp.int32)
    face_vals = common[face_key, axis_ids[None, :]]
    face_vals = jnp.where((slot_links >= 0)[:, :, None, None], face_vals, edge)
    flattened = jnp.transpose(face_vals, (0, 2, 1, 3)).reshape(NSUB, MODES, FACES * CAP)
    codes = jnp.clip(iface_map, 0, FACES * CAP - 1).astype(jnp.int32)
    gather_index = jnp.broadcast_to(codes[:, None, :], (NSUB, MODES, NMAX))
    picked = jnp.take_along_axis(flattened, gather_index, axis=2)
    return (picked + 0.25 * own).astype(jnp.float32)


def draw_dual_blocks(key, part):
    slot_keys = jax.random.split(jax.random.fold_in(key, 7302), NSUB)
    spread = 0.3 / math.sqrt(NMAX)

    def single(slot_key):
        key_off, key_diag = jax.random.split(slot_key)
        entries = jax.random.normal(key_off, (NMAX, NMAX), jnp.float32)
        symmetric = (entries + entries.T) * (spread / math.sqrt(2.0))
        diag_vals = jax.random.uniform(key_diag, (NMAX,), jnp.float32, 1.0, 1.5)
        return (symmetric + jnp.diag(diag_vals)).astype(jnp.bfloat16)
    return jax.lax.map(single, slot_keys)


def block_levels(stream_key, shape, shards, smallest, largest):
    loudness, own = 1.0, jax.random.fold_in(stream_key, 6)
    for dim, shards_of in shards:
        steps = jnp.exp(jax.random.uniform(jax.random.fold_in(own, dim), (shards_of,), jnp.float32, smallest / len(shards), largest / len(shards)))
        loudness = loudness * jnp.repeat(steps, shape[dim] // shards_of).reshape([-1 if axis == dim else 1 for axis in range(len(shape))])
    return loudness


def normal_values(stream_key, extent, scale, bound, cuts=(), kind=jnp.bfloat16):
    values = scale * jax.random.normal(stream_key, extent, jnp.float32)
    if cuts:
        values = values * block_levels(stream_key, extent, cuts, -0.22, 0.18)
    return jnp.clip(values, -bound, bound).astype(kind)


def setup_inputs(seed: int = 0) -> dict:
    key_list = jax.random.split(jax.random.key(seed), 10)
    dual_blocks = draw_dual_blocks(jax.random.fold_in(key_list[9], 71), 0)
    rigid_modes = draw_rigid_modes(jax.random.fold_in(key_list[9], 71), 0)
    dual_local = normal_values(key_list[2], (NSUB, LOADS, NMAX), 1.0, 6.0, ((0, 32),), jnp.float32)
    coarse_rhs = normal_values(key_list[3], (NSUB, MODES, LOADS), (NMAX // 4), 4608.0, ((0, 32),), jnp.float32)
    iface_sizes = draw_iface_sizes(jax.random.fold_in(key_list[9], 71), 0)
    neighbours = draw_neighbours(jax.random.fold_in(key_list[9], 71), 0)
    shared_counts = draw_shared_counts(jax.random.fold_in(key_list[9], 71), 0)
    iface_map = draw_iface_map(jax.random.fold_in(key_list[9], 71), 0)
    owner = draw_owner(jax.random.fold_in(key_list[9], 71), 0)
    return {"dual_blocks": dual_blocks, "rigid_modes": rigid_modes, "dual_local": dual_local, "coarse_rhs": coarse_rhs, "iface_sizes": iface_sizes, "neighbours": neighbours, "shared_counts": shared_counts, "iface_map": iface_map, "owner": owner}


OPPOSITE = (1, 0, 3, 2, 5, 4)
HIGHEST_PRECISION = lax.Precision.HIGHEST

def tables(iface_sizes, neighbours, shared_counts, iface_map, owner):
    columns = jnp.arange(NMAX, dtype=jnp.int32)
    live_dofs = columns[None, :] < iface_sizes[:, None]
    dof_codes = jnp.clip(jnp.where(live_dofs, iface_map, 0), 0, FACES * CAP - 1).astype(jnp.int32)
    which_face = dof_codes // CAP
    position = dof_codes % CAP
    face_owner = jnp.take_along_axis(neighbours, which_face, axis=1)
    face_count = jnp.take_along_axis(shared_counts, which_face, axis=1)
    shared = live_dofs & (face_owner >= 0) & (position < face_count)
    weights = jnp.where(shared, 0.5, jnp.where(live_dofs, 1.0, 0.0)).astype(jnp.float32)
    row_index = jnp.broadcast_to(jnp.arange(NSUB, dtype=jnp.int32)[:, None], (NSUB, NMAX))
    targets = jnp.where(live_dofs, dof_codes, FACES * CAP).astype(jnp.int32)
    inverse = jnp.full((NSUB, FACES * CAP), NMAX, jnp.int32)
    inverse = inverse.at[row_index, targets].set(jnp.broadcast_to(columns[None, :], (NSUB, NMAX)), mode='drop')
    partner_slot = jnp.where(neighbours >= 0, owner[jnp.clip(neighbours, 0, NSUB - 1)], 0).astype(jnp.int32)
    face_mask = ((neighbours >= 0)[:, :, None] & (jnp.arange(CAP, dtype=jnp.int32)[None, None, :] < shared_counts[:, :, None])).astype(jnp.float32)
    return (live_dofs, dof_codes, shared, weights, inverse, partner_slot, face_mask)

def to_faces(values, inverse):
    padded = jnp.concatenate([values, jnp.zeros((values.shape[0], values.shape[1], 1), values.dtype)], axis=2)
    gather_index = jnp.broadcast_to(inverse[:, None, :], (values.shape[0], values.shape[1], FACES * CAP))
    return jnp.take_along_axis(padded, gather_index, axis=2).reshape(values.shape[0], values.shape[1], FACES, CAP)

def partner_faces(face_vals, partner_slot, face_mask):
    opposite = jnp.array(OPPOSITE, jnp.int32)
    swapped = jnp.transpose(face_vals, (0, 2, 1, 3))
    picked = swapped[partner_slot, opposite[None, :]]
    return picked * face_mask[:, :, None, :]

def to_dofs(far_faces, dof_codes, shared):
    flattened = jnp.transpose(far_faces, (0, 2, 1, 3)).reshape(far_faces.shape[0], far_faces.shape[2], FACES * CAP)
    gather_index = jnp.broadcast_to(dof_codes[:, None, :], (far_faces.shape[0], far_faces.shape[2], NMAX))
    return jnp.take_along_axis(flattened, gather_index, axis=2) * shared.astype(jnp.float32)[:, None, :]

def assemble(values, layout):
    live_dofs, dof_codes, shared, weights, inverse, partner_slot, face_mask = layout
    far_faces = partner_faces(to_faces(values, inverse), partner_slot, face_mask)
    return live_dofs.astype(jnp.float32)[:, None, :] * (values - to_dofs(far_faces, dof_codes, shared))

def dual_products(dual_blocks, vectors):

    def single(operands):
        dual_block, vector = operands
        return lax.dot_general(vector.astype(jnp.bfloat16).astype(jnp.float32), dual_block.astype(jnp.float32), (((1,), (1,)), ((), ())), preferred_element_type=jnp.float32)
    return lax.map(single, (dual_blocks, vectors))

def solve_coarse(factor, vector):
    middle = lax.linalg.triangular_solve(factor, vector, left_side=True, lower=True)
    return lax.linalg.triangular_solve(factor, middle, left_side=True, lower=True, transpose_a=True)

def weighted_inner(weights, left_vec, right_vec):
    return jnp.sum(weights[:, None, :] * left_vec * right_vec, axis=(0, 2))

def reference(dual_blocks, rigid_modes, dual_local, coarse_rhs, iface_sizes, neighbours, shared_counts, iface_map, owner):
    layout = tables(iface_sizes, neighbours, shared_counts, iface_map, owner)
    live_dofs, dof_codes, shared, weights, inverse, partner_slot, face_mask = layout
    live_float = live_dofs.astype(jnp.float32)
    modes_live = rigid_modes * live_float[:, None, :]
    own_modes = to_faces(modes_live, inverse)
    far_modes = partner_faces(own_modes, partner_slot, face_mask)
    diagonal = jnp.einsum('iaj,ibj->iab', modes_live, modes_live, precision=HIGHEST_PRECISION)
    coupling = -jnp.einsum('iafp,ifbp->ifab', own_modes, far_modes, precision=HIGHEST_PRECISION)
    slot_index = jnp.arange(NSUB, dtype=jnp.int32)
    coarse_blocks = jnp.zeros((NSUB, MODES, NSUB, MODES), jnp.float32)
    coarse_blocks = coarse_blocks.at[slot_index, :, slot_index, :].set(diagonal)
    coarse_blocks = coarse_blocks.at[slot_index[:, None], :, partner_slot, :].add(coupling)
    factor = jnp.linalg.cholesky(coarse_blocks.reshape(NSUB * MODES, NSUB * MODES))

    def modes_apply(solution):
        stacked = solution.reshape(NSUB, MODES, LOADS)
        own_part = jnp.einsum('iaj,ial->ilj', modes_live, stacked, precision=HIGHEST_PRECISION)
        return assemble(own_part, layout)

    def project(residual):
        coarse_all = jnp.einsum('iaj,ilj->ial', modes_live, residual, precision=HIGHEST_PRECISION).reshape(NSUB * MODES, LOADS)
        projected = residual - modes_apply(solve_coarse(factor, coarse_all))
        return (projected, weighted_inner(weights, projected, projected))

    def dual_apply(vector):
        return assemble(dual_products(dual_blocks, vector), layout)
    dual_rhs = assemble(dual_local, layout)
    multipliers = modes_apply(solve_coarse(factor, coarse_rhs.reshape(NSUB * MODES, LOADS)))
    residual = dual_rhs - dual_apply(multipliers)
    projected, norm_sq = project(residual)
    direction = projected
    for step_index in range(ITERS):
        applied = dual_apply(direction)
        step_size = norm_sq / weighted_inner(weights, direction, applied)
        multipliers = multipliers + step_size[None, :, None] * direction
        residual = residual - step_size[None, :, None] * applied
        projected, norm_next = project(residual)
        direction = projected + (norm_next / norm_sq)[None, :, None] * direction
        norm_sq = norm_next
    return (multipliers, projected)
```

```python
import functools

import jax
import jax.numpy as jnp
from jax import lax
from jax.experimental import pallas as pl
from jax.experimental.pallas import tpu as pltpu
from jax.sharding import PartitionSpec as P

FACES = 6
MODES = 6
ITERS = 3
ROUNDS = ITERS + 1
LANES = 128
LOW = 256
ROWS = 8
FACE_STEPS = (-1, 1, -4, 4, -16, 16)
BLOCK_STEPS = (0,) + FACE_STEPS
HIGHEST = lax.Precision.HIGHEST
MESH = pl.DeviceIdType.MESH
NN = (((1,), (0,)), ((), ()))
NT = (((1,), (1,)), ((), ()))


def coarse_order(slots):
    apart = []
    for slot in range(slots):
        if all((slot + by) % slots not in apart for by in FACE_STEPS):
            apart.append(slot)
    rest = [slot for slot in range(slots) if slot not in apart]
    first = -(-(len(rest) * MODES + ROWS) // LANES) * LANES
    second = -(-len(apart) * MODES // LANES) * LANES
    return apart, rest, first, second


def high_dot(a, b, dims=NN):
    return lax.dot_general(
        a, b, dims, precision=HIGHEST, preferred_element_type=jnp.float32
    )


def split(value, parts):
    out = []
    for part in range(parts):
        piece = value.astype(jnp.bfloat16)
        out.append(piece)
        if part < parts - 1:
            value = value - piece.astype(jnp.float32)
    return out


def row_sum(value):
    return jnp.sum(value, axis=1, keepdims=True)


class Solver:
    def __init__(self, slots, loads, nmax, cap):
        self.slots, self.loads, self.nmax, self.cap = slots, loads, nmax, cap
        self.apart, self.rest, self.first, self.second = coarse_order(slots)
        self.width = self.first + self.second
        self.rhs_lane = len(self.rest) * MODES
        self.merged = 16 % slots == -16 % slots
        self.ports = FACES - 1 if self.merged else FACES
        self.highs = nmax // LOW

    def span(self, face):
        return slice(face * self.cap, (face + 1) * self.cap)

    def scratch(self):
        f32 = jnp.float32
        n, nmax, width, ports = self.slots, self.nmax, self.width, self.ports
        vector = (ROWS, nmax)
        return dict(
            dual=pltpu.VMEM((nmax, nmax), jnp.bfloat16),
            onehot=pltpu.VMEM((LOW, nmax), jnp.bfloat16),
            stack=pltpu.VMEM((3 * ROWS * self.highs, nmax), jnp.bfloat16),
            codes=pltpu.VMEM((1, nmax), jnp.int32),
            pad=pltpu.VMEM(vector, f32),
            modes=pltpu.VMEM(vector, f32),
            far=pltpu.VMEM(vector, f32),
            rhs=pltpu.VMEM(vector, f32),
            shared=pltpu.VMEM((1, nmax), f32),
            weights=pltpu.VMEM((1, nmax), f32),
            m=pltpu.VMEM(vector, f32),
            w=pltpu.VMEM(vector, f32),
            d=pltpu.VMEM(vector, f32),
            q=pltpu.VMEM(vector, f32),
            s=pltpu.VMEM(vector, f32),
            ydof=pltpu.VMEM(vector, f32),
            y=pltpu.VMEM((ROUNDS,) + vector, f32),
            zface=pltpu.VMEM((ROUNDS + 1, ROWS, self.cap), f32),
            fland=pltpu.VMEM((ROUNDS + 1, ports, ROWS, self.cap), f32),
            tsend=pltpu.VMEM((ROUNDS, ROWS, LANES), f32),
            tland=pltpu.VMEM((ROUNDS, n, ROWS, LANES), f32),
            qsend=pltpu.VMEM((ROWS, width), f32),
            qland=pltpu.VMEM((n, ROWS, width), f32),
            packed=pltpu.VMEM((width, width), f32),
            dense=pltpu.VMEM((self.first, self.first), f32),
            basis=pltpu.VMEM((n * ROWS, width), f32),
            picks=pltpu.VMEM((ROWS * (FACES + 1), n * ROWS), f32),
            dual_sem=pltpu.SemaphoreType.DMA((self.highs,)),
            fsend_sem=pltpu.SemaphoreType.DMA((ROUNDS + 1, ports)),
            frecv_sem=pltpu.SemaphoreType.DMA((ROUNDS + 1, ports)),
            tsend_sem=pltpu.SemaphoreType.DMA((ROUNDS,)),
            trecv_sem=pltpu.SemaphoreType.DMA((ROUNDS,)),
            qsend_sem=pltpu.SemaphoreType.DMA((1,)),
            qrecv_sem=pltpu.SemaphoreType.DMA((1,)),
        )


    def prepare_codes(self, sizes_ref, map_ref):
        x = self.x
        columns = lax.broadcasted_iota(jnp.int32, (1, self.nmax), 1)
        x.codes[...] = jnp.where(columns < sizes_ref[0], map_ref[...], -1)

        def body(block, carry):
            at = pl.ds(pl.multiple_of(block * LANES, LANES), LANES)
            codes = x.codes[:, at]
            low = jnp.where(codes < 0, -1, jnp.bitwise_and(codes, LOW - 1))
            rows = lax.broadcasted_iota(jnp.int32, (LOW, LANES), 0)
            x.onehot[:, at] = jnp.where(rows == low, 1.0, 0.0).astype(jnp.bfloat16)
            return carry

        lax.fori_loop(0, self.nmax // LANES, body, 0)

    def to_face(self, source, store, parts):
        x, rows = self.x, ROWS * self.highs

        def body(block, carry):
            at = pl.ds(pl.multiple_of(block * LOW, LOW), LOW)
            high = jnp.right_shift(x.codes[:, at], 8)
            for index, piece in enumerate(split(source[:, at], parts)):
                piece = piece.astype(jnp.float32)
                stacked = [jnp.where(high == h, piece, 0.0) for h in range(self.highs)]
                x.stack[index * rows : (index + 1) * rows, at] = jnp.concatenate(
                    stacked, axis=0
                ).astype(jnp.bfloat16)
            return carry

        lax.fori_loop(0, self.highs, body, 0)
        found = lax.dot_general(
            x.stack[: parts * rows, :], x.onehot[...], NT, preferred_element_type=jnp.float32
        )
        total = found[:rows]
        for index in range(1, parts):
            total = total + found[index * rows : (index + 1) * rows]
        for h in range(self.highs):
            store(h, total[h * ROWS : (h + 1) * ROWS])

    def to_dof(self, source, store, parts):
        x, rows = self.x, ROWS * self.highs
        pieces = [split(source[:, h * LOW : (h + 1) * LOW], parts) for h in range(self.highs)]
        stacked = jnp.concatenate(
            [pieces[h][index].astype(jnp.float32) for index in range(parts)
             for h in range(self.highs)], axis=0,
        ).astype(jnp.bfloat16)
        for block in range(self.highs):
            at = slice(block * LOW, (block + 1) * LOW)
            found = jnp.dot(stacked, x.onehot[:, at], preferred_element_type=jnp.float32)
            total = found[:rows]
            for index in range(1, parts):
                total = total + found[index * rows : (index + 1) * rows]
            high = jnp.right_shift(x.codes[:, at], 8)
            picked = jnp.zeros((ROWS, LOW), jnp.float32)
            for h in range(self.highs):
                picked = jnp.where(high == h, total[h * ROWS : (h + 1) * ROWS], picked)
            store(at, picked)


    def others(self, act):
        def body(by, carry):
            act(lax.rem(self.me + by, self.slots))
            return carry

        lax.fori_loop(1, self.slots, body, 0)

    def face_copies(self, phase, source):
        x = self.x
        copies = []
        for port in range(self.ports):
            merged = self.merged and port == self.ports - 1
            opposite = port if merged else port ^ 1
            target = lax.rem(self.me + FACE_STEPS[port] + self.slots, self.slots)
            copies.append(pltpu.make_async_remote_copy(
                src_ref=x.zface.at[phase] if merged else source(port),
                dst_ref=x.fland.at[phase, opposite],
                send_sem=x.fsend_sem.at[phase, port],
                recv_sem=x.frecv_sem.at[phase, opposite],
                device_id=(target,),
                device_id_type=MESH,
            ))
        return copies

    def start_faces(self, phase, ref):
        x = self.x
        if self.merged:
            lower, upper = self.span(FACES - 2), self.span(FACES - 1)
            x.zface[phase] = jnp.where(x.shared[:, lower] > 0.0, ref[:, lower], ref[:, upper])
        copies = self.face_copies(phase, lambda face: ref.at[:, self.span(face)])
        for copy in copies:
            copy.start()
        return copies

    def far_face(self, phase, face):
        return self.x.fland[phase, min(face, self.ports - 1)] * self.x.shared[:, self.span(face)]

    def all_copy(self, source, landing, send_sem, recv_sem, target):
        return pltpu.make_async_remote_copy(
            src_ref=source, dst_ref=landing, send_sem=send_sem, recv_sem=recv_sem,
            device_id=(target,), device_id_type=MESH,
        )

    def send_all(self, source, landing, send_sem, recv_sem):
        self.others(lambda target: self.all_copy(
            source, landing.at[self.me], send_sem, recv_sem, target
        ).start())

    def wait_all(self, landing, send_sem, recv_sem):
        part = landing.at[pl.ds(0, self.slots - 1)]
        target = lax.rem(self.me + 1, self.slots)
        whole = self.all_copy(part, part, send_sem, recv_sem, target)
        whole.wait_recv()
        whole.wait_send()


    def own_inverse(self, block):
        lane = lax.broadcasted_iota(jnp.int32, (1, LANES), 1)
        sub = lax.broadcasted_iota(jnp.int32, (ROWS, 1), 0)
        for k in range(MODES):
            here = lane == k
            row, column = block[k : k + 1, :], block[:, k : k + 1]
            scale = 1.0 / block[k : k + 1, k : k + 1]
            use = row * scale
            fresh = jnp.where(here, column * scale, block - column * use)
            block = jnp.where(sub == k, jnp.where(here, -scale, use), fresh)
        return -block

    def coarse_row(self, table_ref, rhs_row_ref):
        x, n = self.x, self.slots
        lane = lax.broadcasted_iota(jnp.int32, (1, LANES), 1)
        own = jnp.zeros((ROWS, LANES), jnp.float32)
        for b in range(MODES):
            own = jnp.where(lane == b, row_sum(x.modes[...] * x.modes[b : b + 1, :]), own)
        inverse = self.own_inverse(own)
        laneslot, lanemode = table_ref[0:1, :], table_ref[1:2, :]
        far = jnp.zeros((ROWS, self.width), jnp.float32)
        for face in range(FACES):
            span = self.span(face)
            there = laneslot == lax.rem(self.me + FACE_STEPS[face] + n, n)
            for b in range(MODES):
                value = row_sum(x.modes[:, span] * x.far[b : b + 1, span])
                far -= jnp.where(there & (lanemode == b), value, 0.0)
        here = laneslot == self.me
        scaled = jnp.zeros((ROWS, self.width), jnp.float32)
        plain = far
        for b in range(MODES):
            scaled += inverse[:, b : b + 1] * far[b : b + 1, :]
            at = here & (lanemode == b)
            scaled += jnp.where(at, inverse[:, b : b + 1], 0.0)
            plain += jnp.where(at, own[:, b : b + 1], 0.0)
        apart = sum((self.me == slot).astype(jnp.int32) for slot in self.apart)
        x.qsend[...] = jnp.where(apart > 0, scaled, plain) + rhs_row_ref[...]

    def eliminate(self):
        out = self.x.dense
        lane = lax.broadcasted_iota(jnp.int32, (1, self.first), 1)

        def body(step, carry):
            k = 2 * step
            at0, at1 = lane == k, lane == k + 1
            row0 = out[pl.ds(k, 1), :]
            row1 = out[pl.ds(k + 1, 1), :]
            p00 = row_sum(jnp.where(at0, row0, 0.0))
            p01 = row_sum(jnp.where(at1, row0, 0.0))
            p11 = row_sum(jnp.where(at1, row1, 0.0))
            first = 1.0 / p00
            ratio = p01 * first
            i11 = 1.0 / (p11 - p01 * ratio)
            i01 = -ratio * i11
            i00 = first + ratio * ratio * i11
            use0 = i00 * row0 + i01 * row1
            use1 = i01 * row0 + i11 * row1
            whole = out[...]
            col0 = row_sum(jnp.where(at0, whole, 0.0))
            col1 = row_sum(jnp.where(at1, whole, 0.0))
            fresh = whole - col0 * use0 - col1 * use1
            fresh = jnp.where(at0, col0 * i00 + col1 * i01, fresh)
            fresh = jnp.where(at1, col0 * i01 + col1 * i11, fresh)
            out[...] = fresh
            out[pl.ds(k, 1), :] = jnp.where(at0, -i00, jnp.where(at1, -i01, use0))
            out[pl.ds(k + 1, 1), :] = jnp.where(at0, -i01, jnp.where(at1, -i11, use1))
            return carry

        lax.fori_loop(0, len(self.rest) * MODES // 2, body, 0)

    def coarse_inverse(self, table_ref):
        x, n, first = self.x, self.slots, self.first
        x.packed[...] = jnp.zeros(x.packed.shape, jnp.float32)
        for start, group in ((0, self.rest), (first, self.apart)):
            for place, slot in enumerate(group):
                at = start + place * MODES
                x.packed[at : at + MODES, :] = x.qland[slot, :MODES, :]
        x.dense[...] = x.packed[:first, :first] - high_dot(
            x.packed[:first, first:], x.packed[first:, :first]
        )
        self.eliminate()
        laneslot, lanemode = table_ref[0:1, :], table_ref[1:2, :]
        lane = lax.broadcasted_iota(jnp.int32, (1, self.width), 1)
        sub = lax.broadcasted_iota(jnp.int32, (ROWS, 1), 0)
        for slot in range(n):
            unit = jnp.where((laneslot == slot) & (lanemode == sub), 1.0, 0.0)
            if slot in self.apart:
                unit -= jnp.where(lane < self.rhs_lane, x.qland[slot], 0.0)
            x.basis[slot * ROWS : (slot + 1) * ROWS, :] = unit
        chosen = jnp.concatenate([
            x.basis[pl.ds(pl.multiple_of(lax.rem(self.me + by + n, n) * ROWS, ROWS), ROWS), :]
            for by in BLOCK_STEPS
        ], axis=0)
        solved = jnp.concatenate([
            -high_dot(chosen[:, :first], x.dense[...]),
            high_dot(chosen[:, first:], x.packed[first:, first:]),
        ], axis=1)
        x.picks[...] = high_dot(solved, x.basis[...], NT)

    def columns(self, found, mask):
        return [
            [row_sum(found[g * ROWS + a : g * ROWS + a + 1, :] * mask) for a in range(MODES)]
            for g in range(FACES + 1)
        ]

    def rigid_part(self, z, face):
        x, span = self.x, self.span(face)
        total = jnp.zeros((ROWS, self.cap), jnp.float32)
        for a in range(MODES):
            total += z[0][a] * x.modes[a : a + 1, span]
            total -= z[face + 1][a] * x.far[a : a + 1, span]
        return total


    def product(self, vector, store):
        x = self.x
        wide = 512
        x.stack[:ROWS, :] = jnp.zeros((ROWS, self.nmax), jnp.bfloat16)

        def keep(at, block):
            x.stack[:ROWS, at] = block.astype(jnp.bfloat16)

        self.to_dof(vector, keep, 1)

        def body(block, carry):
            at = pl.ds(pl.multiple_of(block * wide, wide), wide)
            x.ydof[:, at] = jnp.dot(
                x.stack[:ROWS, :], x.dual[:, at], preferred_element_type=jnp.float32
            )
            return carry

        lax.fori_loop(0, self.nmax // wide, body, 0)
        self.to_face(x.ydof, store, 2)

    def contributions(self, ref, scalars):
        x = self.x
        lane = lax.broadcasted_iota(jnp.int32, (ROWS, LANES), 1)
        sub = lax.broadcasted_iota(jnp.int32, (ROWS, LANES), 0)
        out = jnp.zeros((ROWS, LANES), jnp.float32)
        for load in range(self.loads):
            own = jnp.zeros((ROWS, self.cap), jnp.float32)
            for face in range(FACES):
                span = self.span(face)
                row = ref[load : load + 1, span]
                own += x.modes[:, span] * row
                other = row_sum(x.far[:, span] * row)
                out = jnp.where(lane == load * ROWS + face + 1, -other, out)
            out = jnp.where(lane == load * ROWS, row_sum(own), out)
        if scalars:
            spread = jnp.zeros((ROWS, LANES), jnp.float32)
            for index, value in enumerate(scalars):
                spread = jnp.where(lane == sub * ROWS + index, value, spread)
            out = jnp.where(sub == MODES, jnp.sum(spread, axis=0, keepdims=True), out)
        return out

    def collect(self, phase):
        x, n = self.x, self.slots
        lane = lax.broadcasted_iota(jnp.int32, (ROWS, LANES), 1)
        sub = lax.broadcasted_iota(jnp.int32, (ROWS, LANES), 0)
        group = jnp.bitwise_and(lane, ROWS - 1)
        total = x.tland[phase, 0]
        for slot in range(1, n):
            total = total + x.tland[phase, slot]
        merged = []
        for slot in range(n):
            value = x.tland[phase, slot]
            for face in range(FACES):
                sender = (slot - FACE_STEPS[face]) % n
                value = jnp.where(group == face + 1, x.tland[phase, sender], value)
            merged.append(value)
        found = high_dot(x.picks[...], jnp.concatenate(merged, axis=0))
        z = self.columns(found, jnp.where(jnp.right_shift(lane, 3) == sub, 1.0, 0.0))
        sums = [
            row_sum(jnp.where(lane == sub * ROWS + i, total[MODES : MODES + 1, :], 0.0))
            for i in range(4)
        ]
        return z, sums

    def communicate(self, phase, ref, scalars):
        x = self.x
        copies = self.start_faces(phase + 1, ref)
        x.tsend[phase] = self.contributions(ref, scalars)
        landing = x.tland.at[phase]
        self.send_all(x.tsend.at[phase], landing, x.tsend_sem.at[phase], x.trecv_sem.at[phase])
        x.tland[phase, self.me] = x.tsend[phase]
        self.wait_all(landing, x.tsend_sem.at[phase], x.trecv_sem.at[phase])
        for copy in copies:
            copy.wait()


    def run(self, sizes_ref, neighbours_ref, counts_ref, map_ref, modes_ref, local_ref,
            rhs_row_ref, table_ref, dual_ref, mult_out, resid_out, x):
        self.x = x
        self.me = lax.axis_index("dev")
        n, f32 = self.slots, jnp.float32
        loads = []
        for block in range(self.highs):
            at = pl.ds(block * LOW, LOW)
            copy = pltpu.make_async_copy(
                dual_ref.at[0, at, :], x.dual.at[at, :], x.dual_sem.at[block]
            )
            copy.start()
            loads.append(copy)
        barrier = pltpu.get_barrier_semaphore()
        self.others(lambda target: pl.semaphore_signal(
            barrier, inc=1, device_id=(target,), device_id_type=MESH
        ))

        self.prepare_codes(sizes_ref, map_ref)
        place = lax.broadcasted_iota(jnp.int32, (1, self.cap), 1)
        for face in range(FACES):
            counted = jnp.where(place < counts_ref[0, face], 1.0, 0.0)
            both = jnp.where(neighbours_ref[0, face] >= 0, counted, jnp.zeros_like(counted))
            x.shared[:, self.span(face)] = both
            x.weights[:, self.span(face)] = counted - 0.5 * both
        x.pad[...] = jnp.zeros((ROWS, self.nmax), f32)
        x.pad[:MODES, :] = modes_ref[0]

        def keep(ref):
            def store(high, block):
                ref[:, high * LOW : (high + 1) * LOW] = block
            return store

        self.to_face(x.pad, keep(x.modes), 3)
        pl.semaphore_wait(barrier, n - 1)
        copies = self.start_faces(0, x.modes)
        self.to_face(local_ref.at[0], keep(x.rhs), 3)
        for copy in copies:
            copy.wait()
        for face in range(FACES):
            x.far[:, self.span(face)] = self.far_face(0, face)
        self.coarse_row(table_ref, rhs_row_ref)
        self.send_all(x.qsend, x.qland, x.qsend_sem.at[0], x.qrecv_sem.at[0])
        x.qland[self.me] = x.qsend[...]
        self.wait_all(x.qland, x.qsend_sem.at[0], x.qrecv_sem.at[0])
        self.coarse_inverse(table_ref)

        tile = self.rhs_lane // LANES * LANES
        goal = x.qland[:, :, tile : tile + LANES].reshape(n * ROWS, LANES)
        lane = lax.broadcasted_iota(jnp.int32, (ROWS, LANES), 1)
        sub = lax.broadcasted_iota(jnp.int32, (ROWS, LANES), 0)
        mask = jnp.where(lane == sub + (self.rhs_lane - tile), 1.0, 0.0)
        goal = jnp.where(lane[0:1] >= self.rhs_lane - tile, goal, 0.0)
        z = self.columns(high_dot(x.picks[...], goal), mask)
        for face in range(FACES):
            x.m[:, self.span(face)] = self.rigid_part(z, face)
        for copy in loads:
            copy.wait()

        def first_store(high, block):
            at = slice(high * LOW, (high + 1) * LOW)
            x.y[0, :, at] = x.rhs[:, at] - block

        self.product(x.m, first_store)
        self.communicate(0, x.y.at[0], None)
        z, _ = self.collect(0)
        for face in range(FACES):
            span = self.span(face)
            x.w[:, span] = x.y[0, :, span] - self.far_face(1, face) - self.rigid_part(z, face)

        for phase in range(1, ROUNDS):
            self.product(x.w, keep(x.y.at[phase]))
            w, y = x.w[...], x.y[phase]
            weighted = w * x.weights[...]
            zero = jnp.zeros((ROWS, 1), f32)
            scalars = [
                row_sum(weighted * w),
                row_sum(w * y),
                row_sum(weighted * x.q[...]) if phase > 1 else zero,
                row_sum(x.d[...] * y) if phase > 1 else zero,
            ]
            self.communicate(phase, x.y.at[phase], scalars)
            z, (rho, wa, wq, da) = self.collect(phase)
            if phase > 1:
                beta = rho / rho_old
                curve = wa + beta * (wq + da) + beta * beta * curve
            else:
                beta, curve = None, wa
            step = rho / curve
            rho_old = rho
            for face in range(FACES):
                span = self.span(face)
                applied = x.y[phase, :, span] - self.far_face(phase + 1, face)
                d, q, s = x.w[:, span], applied, applied - self.rigid_part(z, face)
                if phase > 1:
                    d += beta * x.d[:, span]
                    q += beta * x.q[:, span]
                    s += beta * x.s[:, span]
                x.m[:, span] += step * d
                x.w[:, span] -= step * s
                if phase < ITERS:
                    x.d[:, span], x.q[:, span], x.s[:, span] = d, q, s

        for ref, out in ((x.m, mult_out), (x.w, resid_out)):
            def put(at, block, out=out):
                out[0, :, at] = block
            self.to_dof(ref, put, 3)


class Refs:
    def __init__(self, names, refs):
        self.__dict__.update(zip(names, refs))


def per_device(
    dual_blocks, rigid_modes, dual_local, coarse_rhs, iface_sizes, neighbours, shared_counts,
    iface_map, owner,
):
    slots = lax.axis_size("dev")
    loads, nmax = dual_local.shape[1:]
    solver = Solver(slots, loads, nmax, nmax // FACES)
    scratch = solver.scratch()
    names = list(scratch)

    def kernel(*refs):
        solver.run(*refs[:11], Refs(names, refs[11:]))

    laneslot, lanemode = [-1] * solver.width, [-1] * solver.width
    for start, group in ((0, solver.rest), (solver.first, solver.apart)):
        for place, slot in enumerate(group):
            for mode in range(MODES):
                laneslot[start + place * MODES + mode] = slot
                lanemode[start + place * MODES + mode] = mode
    table = jnp.array([laneslot, lanemode] + [[0] * solver.width] * 6, jnp.int32)
    left = solver.rhs_lane
    rhs_row = jnp.pad(
        coarse_rhs[0], ((0, ROWS - MODES), (left, solver.width - left - loads))
    )
    vmem, smem = pl.BlockSpec(memory_space=pltpu.VMEM), pl.BlockSpec(memory_space=pltpu.SMEM)
    result = jax.ShapeDtypeStruct((1, loads, nmax), jnp.float32)
    return pl.pallas_call(
        kernel,
        out_shape=(result, result),
        in_specs=[smem] * 3 + [vmem] * 5 + [pl.BlockSpec(memory_space=pl.ANY)],
        out_specs=(vmem, vmem),
        scratch_shapes=list(scratch.values()),
        compiler_params=pltpu.CompilerParams(
            collective_id=0, has_side_effects=True, vmem_limit_bytes=58 * 2**20
        ),
    )(
        iface_sizes, neighbours, shared_counts, iface_map, rigid_modes, dual_local, rhs_row,
        table, dual_blocks,
    )


def solution(mesh):
    return jax.shard_map(
        per_device,
        mesh=mesh,
        in_specs=(
            P("dev", None, None),
            P("dev", None, None),
            P("dev", None, None),
            P("dev", None, None),
            P("dev"),
            P("dev", None),
            P("dev", None),
            P("dev", None),
            P(),
        ),
        out_specs=(P("dev", None, None), P("dev", None, None)),
        check_vma=False,
    )
```

```python
import functools

import jax
import jax.numpy as jnp
from jax import lax
from jax.experimental import pallas as pl
from jax.experimental.pallas import tpu as pltpu
from jax.sharding import PartitionSpec as P

FACES = 6
MODES = 6
ITERS = 3
ROUNDS = ITERS + 1
LANES = 128
HALF = 64
WIDE = 1536
LOW = 256
ROWS = 8
FACE_STEPS = (-1, 1, -4, 4, -16, 16)
BLOCK_STEPS = (0,) + FACE_STEPS
HIGHEST = lax.Precision.HIGHEST
MESH = pl.DeviceIdType.MESH
NN = (((1,), (0,)), ((), ()))
NT = (((1,), (1,)), ((), ()))


def coarse_order(slots):
    apart = []
    for slot in range(slots):
        if all((slot + by) % slots not in apart for by in FACE_STEPS):
            apart.append(slot)
    rest = [slot for slot in range(slots) if slot not in apart]
    first = -(-len(rest) * MODES // LANES) * LANES
    second = -(-len(apart) * MODES // LANES) * LANES
    return apart, rest, first, second


def high_dot(a, b, dims=NN):
    return lax.dot_general(
        a, b, dims, precision=HIGHEST, preferred_element_type=jnp.float32
    )


def split(value, parts):
    out = []
    for part in range(parts):
        piece = value.astype(jnp.bfloat16)
        out.append(piece)
        if part < parts - 1:
            value = value - piece.astype(jnp.float32)
    return out


def row_sum(value):
    return jnp.sum(value, axis=1, keepdims=True)


class Solver:
    def __init__(self, slots, loads, nmax, cap):
        self.slots, self.loads, self.nmax, self.cap = slots, loads, nmax, cap
        self.apart, self.rest, self.first, self.second = coarse_order(slots)
        self.width = self.first + self.second
        self.lane_of = {}
        for start, group in ((0, self.rest), (self.first, self.apart)):
            for place, slot in enumerate(group):
                self.lane_of[slot] = start + place * MODES
        self.merged = 16 % slots == -16 % slots
        self.ports = FACES - 1 if self.merged else FACES
        self.highs = nmax // LOW

    def span(self, face):
        return slice(face * self.cap, (face + 1) * self.cap)

    def scratch(self):
        f32 = jnp.float32
        n, nmax, width, ports = self.slots, self.nmax, self.width, self.ports
        vector = (ROWS, nmax)
        return dict(
            dual=pltpu.VMEM((nmax, nmax), jnp.bfloat16),
            onehot=pltpu.VMEM((LOW, nmax), jnp.bfloat16),
            stack=pltpu.VMEM((3 * ROWS * self.highs, nmax), jnp.bfloat16),
            codes=pltpu.VMEM((1, nmax), jnp.int32),
            places=pltpu.VMEM((1, nmax), jnp.int32),
            unhot=pltpu.VMEM((LOW, nmax), jnp.bfloat16),
            small=pltpu.VMEM((ROWS, LANES), f32),
            own=pltpu.VMEM((2, ROWS, LANES), f32),
            pad=pltpu.VMEM(vector, f32),
            modes=pltpu.VMEM(vector, f32),
            far=pltpu.VMEM(vector, f32),
            shared=pltpu.VMEM((1, nmax), f32),
            weights=pltpu.VMEM((1, nmax), f32),
            counted=pltpu.VMEM((1, nmax), f32),
            m=pltpu.VMEM(vector, f32),
            w=pltpu.VMEM(vector, f32),
            d=pltpu.VMEM(vector, f32),
            q=pltpu.VMEM(vector, f32),
            s=pltpu.VMEM(vector, f32),
            a=pltpu.VMEM(vector, f32),
            dofs=pltpu.VMEM(vector, f32),
            yfresh=pltpu.VMEM(vector, f32),
            yw=pltpu.VMEM(vector, f32),
            ys=pltpu.VMEM(vector, f32),
            yrigid=pltpu.VMEM((ROWS * (FACES + 1), nmax), f32),
            y=pltpu.VMEM((ROUNDS,) + vector, f32),
            zface=pltpu.VMEM((ROUNDS + 1, ROWS, self.cap), f32),
            fland=pltpu.VMEM((ROUNDS + 1, ports, ROWS, self.cap), f32),
            tsend=pltpu.VMEM((ROUNDS + 1, ROWS // 2, LANES), f32),
            tland=pltpu.VMEM((ROUNDS + 1, n, ROWS // 2, LANES), f32),
            merged=pltpu.VMEM((n * ROWS // 2, LANES), f32),
            qrows=pltpu.VMEM((n, ROWS, width), f32),
            packed=pltpu.VMEM((width, width), f32),
            dense=pltpu.VMEM((self.first, self.first), f32),
            basis=pltpu.VMEM((n * ROWS, width), f32),
            halves=pltpu.VMEM((2, n * ROWS // 2, width), f32),
            picks=pltpu.VMEM((2 * ROWS * (FACES + 1), n * ROWS // 2), f32),
            map=pltpu.VMEM((1, nmax), jnp.int32),
            raw=pltpu.VMEM((MODES, 1, nmax), f32),
            local=pltpu.VMEM((1, self.loads, nmax), f32),
            goal=pltpu.VMEM((MODES, 1, self.loads), f32),
            table=pltpu.VMEM((ROWS, width), jnp.int32),
            links=pltpu.SMEM((1, FACES), jnp.int32),
            counts=pltpu.SMEM((1, FACES), jnp.int32),
            in_sem=pltpu.SemaphoreType.DMA((7,)),
            dual_sem=pltpu.SemaphoreType.DMA((self.highs,)),
            fsend_sem=pltpu.SemaphoreType.DMA((ROUNDS + 1, ports)),
            frecv_sem=pltpu.SemaphoreType.DMA((ROUNDS + 1, ports)),
            tsend_sem=pltpu.SemaphoreType.DMA((ROUNDS + 1,)),
            trecv_sem=pltpu.SemaphoreType.DMA((ROUNDS + 1,)),
        )


    def spread_low(self, codes_ref, onehot_ref):
        def body(block, carry):
            at = pl.ds(pl.multiple_of(block * LANES, LANES), LANES)
            codes = codes_ref[:, at]
            low = jnp.where(codes < 0, -1, jnp.bitwise_and(codes, LOW - 1))
            rows = lax.broadcasted_iota(jnp.int32, (LOW, LANES), 0)
            onehot_ref[:, at] = jnp.where(rows == low, 1.0, 0.0).astype(jnp.bfloat16)
            return carry

        lax.fori_loop(0, self.nmax // LANES, body, 0)

    def scatter_modes(self):
        x, rows, parts = self.x, ROWS * self.highs, 3

        def body(block, carry):
            at = pl.ds(pl.multiple_of(block * LOW, LOW), LOW)
            high = jnp.right_shift(x.codes[:, at], 8)
            for index, piece in enumerate(split(x.pad[:, at], parts)):
                piece = piece.astype(jnp.float32)
                stacked = [jnp.where(high == h, piece, 0.0) for h in range(self.highs)]
                x.stack[index * rows : (index + 1) * rows, at] = jnp.concatenate(
                    stacked, axis=0
                ).astype(jnp.bfloat16)
            return carry

        lax.fori_loop(0, self.highs, body, 0)
        found = lax.dot_general(
            x.stack[...], x.onehot[...], NT, preferred_element_type=jnp.float32
        )
        total = found[:rows] + found[rows : 2 * rows] + found[2 * rows :]
        sub = lax.broadcasted_iota(jnp.int32, (ROWS, LOW), 0)
        for h in range(self.highs):
            at = slice(h * LOW, (h + 1) * LOW)
            block = total[h * ROWS : (h + 1) * ROWS]
            x.modes[:, at] = jnp.where(sub < MODES, block, 0.0)
            place = block[MODES : MODES + 1] * LOW + block[MODES + 1 : MODES + 2]
            place = (place + 0.5).astype(jnp.int32)
            x.places[:, at] = jnp.where(x.counted[:, at] > 0.0, place, -1)

    def reorder(self, source, codes_ref, onehot_ref, parts, store):
        rows = ROWS * self.highs
        pieces = [split(source[:, h * LOW : (h + 1) * LOW], parts) for h in range(self.highs)]
        stacked = jnp.concatenate(
            [pieces[h][index].astype(jnp.float32) for index in range(parts)
             for h in range(self.highs)], axis=0,
        ).astype(jnp.bfloat16)
        for block in range(self.highs):
            at = slice(block * LOW, (block + 1) * LOW)
            found = jnp.dot(stacked, onehot_ref[:, at], preferred_element_type=jnp.float32)
            total = found[:rows]
            for index in range(1, parts):
                total = total + found[index * rows : (index + 1) * rows]
            high = jnp.right_shift(codes_ref[:, at], 8)
            picked = jnp.zeros((ROWS, LOW), jnp.float32)
            for h in range(self.highs):
                picked = jnp.where(high == h, total[h * ROWS : (h + 1) * ROWS], picked)
            store(at, picked)

    def to_dof(self, source, parts, store):
        self.reorder(source, self.x.codes, self.x.onehot, parts, store)

    def to_face(self, source, parts, store):
        self.reorder(source, self.x.places, self.x.unhot, parts, store)


    def others(self, act):
        def body(by, carry):
            act(lax.rem(self.me + by, self.slots))
            return carry

        lax.fori_loop(1, self.slots, body, 0)

    def face_copies(self, phase, source):
        x = self.x
        copies = []
        for port in range(self.ports):
            merged = self.merged and port == self.ports - 1
            opposite = port if merged else port ^ 1
            target = lax.rem(self.me + FACE_STEPS[port] + self.slots, self.slots)
            copies.append(pltpu.make_async_remote_copy(
                src_ref=x.zface.at[phase] if merged else source(port),
                dst_ref=x.fland.at[phase, opposite],
                send_sem=x.fsend_sem.at[phase, port],
                recv_sem=x.frecv_sem.at[phase, opposite],
                device_id=(target,),
                device_id_type=MESH,
            ))
        return copies

    def start_faces(self, phase, ref):
        x = self.x
        if self.merged:
            lower, upper = self.span(FACES - 2), self.span(FACES - 1)
            x.zface[phase] = jnp.where(x.shared[:, lower] > 0.0, ref[:, lower], ref[:, upper])
        copies = self.face_copies(phase, lambda face: ref.at[:, self.span(face)])
        for copy in copies:
            copy.start()
        return copies

    def far_face(self, phase, face):
        return self.x.fland[phase, min(face, self.ports - 1)] * self.x.shared[:, self.span(face)]

    def all_copy(self, phase, source, landing, target):
        x = self.x
        return pltpu.make_async_remote_copy(
            src_ref=source, dst_ref=landing, send_sem=x.tsend_sem.at[phase],
            recv_sem=x.trecv_sem.at[phase], device_id=(target,), device_id_type=MESH,
        )

    def send_all(self, phase, tile):
        x = self.x
        lane = lax.broadcasted_iota(jnp.int32, (ROWS // 2, LANES), 1)
        packed = jnp.where(lane < HALF, tile[: ROWS // 2], pltpu.roll(tile, HALF, 1)[ROWS // 2 :])
        x.tsend[phase] = packed
        source, landing = x.tsend.at[phase], x.tland.at[phase, self.me]
        self.others(lambda target: self.all_copy(phase, source, landing, target).start())
        x.tland[phase, self.me] = packed

    def wait_all(self, phase):
        part = self.x.tland.at[phase, pl.ds(0, self.slots - 1)]
        whole = self.all_copy(phase, part, part, lax.rem(self.me + 1, self.slots))
        whole.wait_recv()
        whole.wait_send()


    def own_inverse(self, block):
        lane = lax.broadcasted_iota(jnp.int32, (1, LANES), 1)
        sub = lax.broadcasted_iota(jnp.int32, (ROWS, 1), 0)
        for k in range(MODES):
            here = lane == k
            row, column = block[k : k + 1, :], block[:, k : k + 1]
            scale = 1.0 / block[k : k + 1, k : k + 1]
            use = row * scale
            fresh = jnp.where(here, column * scale, block - column * use)
            block = jnp.where(sub == k, jnp.where(here, -scale, use), fresh)
        return -block

    def own_block(self):
        x = self.x
        lane = lax.broadcasted_iota(jnp.int32, (1, LANES), 1)
        own = jnp.zeros((ROWS, LANES), jnp.float32)
        for b in range(MODES):
            own = jnp.where(lane == b, row_sum(x.modes[...] * x.modes[b : b + 1, :]), own)
        x.own[0], x.own[1] = own, self.own_inverse(own)
        x.small[...] = jnp.zeros((ROWS, LANES), jnp.float32)
        for a in range(MODES):
            x.small[a : a + 1, : self.loads] = x.goal[a]

    def coarse_row(self):
        x = self.x
        lane = lax.broadcasted_iota(jnp.int32, (1, LANES), 1)
        own, inverse = x.own[0], x.own[1]
        far = jnp.zeros((ROWS, LANES), jnp.float32)
        for face in range(FACES):
            span = self.span(face)
            for b in range(MODES):
                value = row_sum(x.modes[:, span] * x.far[b : b + 1, span])
                far = jnp.where(lane == (face + 1) * ROWS + b, -value, far)
        scaled = inverse
        for b in range(MODES):
            scaled += inverse[:, b : b + 1] * far[b : b + 1, :]
        apart = sum((self.me == slot).astype(jnp.int32) for slot in self.apart)
        goal = pltpu.roll(x.small[...], HALF - ROWS, 1)
        return jnp.where(apart > 0, scaled, far + own) + goal

    def spread_rows(self):
        x, n, phase = self.x, self.slots, ROUNDS
        for slot in range(n):
            packed = x.tland[phase, slot]
            tile = jnp.concatenate([packed, pltpu.roll(packed, HALF, 1)], axis=0)
            tiles = [None] * (self.width // LANES)
            for g, by in enumerate(BLOCK_STEPS):
                target = (slot + by) % n
                place = self.lane_of[target]
                for index in {place // LANES, (place + MODES - 1) // LANES}:
                    table = x.table[0:1, index * LANES : (index + 1) * LANES]
                    moved = pltpu.roll(tile, (place - g * ROWS) % LANES, 1)
                    part = jnp.where(table == target, moved, 0.0)
                    tiles[index] = part if tiles[index] is None else tiles[index] + part
            for index, part in enumerate(tiles):
                if part is None:
                    part = jnp.zeros((ROWS, LANES), jnp.float32)
                x.qrows[slot, :, index * LANES : (index + 1) * LANES] = part

    def eliminate(self):
        out = self.x.dense
        lane = lax.broadcasted_iota(jnp.int32, (1, self.first), 1)
        modes = range(MODES)

        def body(step, carry):
            k = step * MODES
            at = [lane == k + a for a in modes]
            rows = [out[pl.ds(k + a, 1), :] for a in modes]
            block = [[None] * MODES for a in modes]
            for a in modes:
                for b in range(a, MODES):
                    block[a][b] = row_sum(jnp.where(at[b], rows[a], 0.0))
                    block[b][a] = block[a][b]
            for c in modes:
                scale = 1.0 / block[c][c]
                column = [block[a][c] for a in modes]
                use = [column[a] * scale for a in modes]
                for a in modes:
                    for b in range(a, MODES):
                        if a == c and b == c:
                            fresh = -scale
                        elif b == c:
                            fresh = use[a]
                        elif a == c:
                            fresh = use[b]
                        else:
                            fresh = block[a][b] - column[a] * use[b]
                        block[a][b] = block[b][a] = fresh
            uses = []
            for a in modes:
                use = -block[a][0] * rows[0]
                for b in range(1, MODES):
                    use -= block[a][b] * rows[b]
                for b in modes:
                    use = jnp.where(at[b], block[a][b], use)
                uses.append(use)
            whole = out[...]
            fresh = jnp.where((lane >= k) & (lane < k + MODES), 0.0, whole)
            for a in modes:
                fresh -= row_sum(jnp.where(at[a], whole, 0.0)) * uses[a]
            out[...] = fresh
            for a in modes:
                out[pl.ds(k + a, 1), :] = uses[a]
            return carry

        lax.fori_loop(0, len(self.rest), body, 0)

    def coarse_inverse(self):
        x, n, first, half = self.x, self.slots, self.first, ROWS // 2
        self.spread_rows()
        x.packed[...] = jnp.zeros(x.packed.shape, jnp.float32)
        for slot in range(n):
            at = self.lane_of[slot]
            x.packed[at : at + MODES, :] = x.qrows[slot, :MODES, :]
        x.dense[...] = x.packed[:first, :first] - high_dot(
            x.packed[:first, first:], x.packed[first:, :first]
        )
        with jax.named_scope("eliminate"):
            self.eliminate()
        laneslot, lanemode = x.table[0:1, :], x.table[1:2, :]
        lane = lax.broadcasted_iota(jnp.int32, (1, self.width), 1)
        sub = lax.broadcasted_iota(jnp.int32, (ROWS, 1), 0)
        for slot in range(n):
            unit = jnp.where((laneslot == slot) & (lanemode == sub), 1.0, 0.0)
            if slot in self.apart:
                unit -= jnp.where((lane < first) & (sub < MODES), x.qrows[slot], 0.0)
            x.basis[slot * ROWS : (slot + 1) * ROWS, :] = unit
            x.halves[0, slot * half : (slot + 1) * half, :] = unit[:half]
            x.halves[1, slot * half : (slot + 1) * half, :] = unit[half:]
        chosen = jnp.concatenate([
            x.basis[pl.ds(pl.multiple_of(lax.rem(self.me + by + n, n) * ROWS, ROWS), ROWS), :]
            for by in BLOCK_STEPS
        ], axis=0)
        solved = jnp.concatenate([
            -high_dot(chosen[:, :first], x.dense[...]),
            high_dot(chosen[:, first:], x.packed[first:, first:]),
        ], axis=1)
        rows = chosen.shape[0]
        x.picks[:rows] = high_dot(solved, x.halves[0], NT)
        x.picks[rows:] = high_dot(solved, x.halves[1], NT)

    def coarse_columns(self, values, left, right):
        found = high_dot(self.x.picks[...], values)
        rows = ROWS * (FACES + 1)
        return [
            [row_sum(found[at : at + 1] * left + found[rows + at : rows + at + 1] * right)
             for at in range(g * ROWS, g * ROWS + MODES)]
            for g in range(FACES + 1)
        ]

    def rigid_part(self, z, face):
        x, span = self.x, self.span(face)
        total = jnp.zeros((ROWS, self.cap), jnp.float32)
        for a in range(MODES):
            total += z[0][a] * x.modes[a : a + 1, span]
            total -= z[face + 1][a] * x.far[a : a + 1, span]
        return total


    def rigid_product(self, z, at):
        total = z[0][0] * self.x.yrigid[0:1, at]
        for g in range(FACES + 1):
            for a in range(MODES):
                if g or a:
                    total += z[g][a] * self.x.yrigid[g * ROWS + a : g * ROWS + a + 1, at]
        return total

    def product(self, rows, out):
        x, wide = self.x, WIDE

        def body(block, carry):
            at = pl.ds(pl.multiple_of(block * wide, wide), wide)
            both = jnp.dot(
                x.stack[: 2 * rows, :], x.dual[:, at], preferred_element_type=jnp.float32
            )
            out[:, at] = both[:rows] + both[rows:]
            return carry

        lax.fori_loop(0, self.nmax // wide, body, 0)

    def stack_vector(self, at, block):
        parts = [piece.astype(jnp.float32) for piece in split(block, 2)]
        self.x.stack[: 2 * ROWS, at] = jnp.concatenate(parts, axis=0).astype(jnp.bfloat16)

    def rigid_products(self):
        x = self.x

        def keep(at, block):
            x.dofs[:, at] = block

        self.to_dof(x.far, 3, keep)
        sub = lax.broadcasted_iota(jnp.int32, (ROWS, LOW), 0)
        for block in range(self.highs):
            at = slice(block * LOW, (block + 1) * LOW)
            codes = x.codes[:, at]
            own = jnp.where((codes >= 0) & (sub < MODES), x.pad[:, at], 0.0)
            own = [piece.astype(jnp.float32) for piece in split(own, 2)]
            far = [piece.astype(jnp.float32) for piece in split(-x.dofs[:, at], 2)]
            rows = []
            for index in range(2):
                rows.append(own[index])
                for face in range(FACES):
                    here = (codes >= face * self.cap) & (codes < (face + 1) * self.cap)
                    rows.append(jnp.where(here, far[index], 0.0))
            x.stack[: len(rows) * ROWS, at] = jnp.concatenate(rows, axis=0).astype(jnp.bfloat16)
        self.product(ROWS * (FACES + 1), x.yrigid)

    def contributions(self, ref, scalars):
        x = self.x
        lane = lax.broadcasted_iota(jnp.int32, (ROWS, LANES), 1)
        sub = lax.broadcasted_iota(jnp.int32, (ROWS, LANES), 0)
        out = jnp.zeros((ROWS, LANES), jnp.float32)
        for load in range(self.loads):
            own = jnp.zeros((ROWS, self.cap), jnp.float32)
            for face in range(FACES):
                span = self.span(face)
                row = ref[load : load + 1, span]
                own += x.modes[:, span] * row
                other = row_sum(x.far[:, span] * row)
                out = jnp.where(lane == load * ROWS + face + 1, -other, out)
            out = jnp.where(lane == load * ROWS, row_sum(own), out)
        if scalars:
            spread = jnp.zeros((ROWS, LANES), jnp.float32)
            for index, value in enumerate(scalars):
                spread = jnp.where(lane == sub * ROWS + index, value, spread)
            out = jnp.where(sub == MODES, jnp.sum(spread, axis=0, keepdims=True), out)
        return out

    def collect(self, phase):
        x, n, half = self.x, self.slots, ROWS // 2
        group = jnp.bitwise_and(lax.broadcasted_iota(jnp.int32, (half, LANES), 1), ROWS - 1)
        total = x.tland[phase, 0]
        for slot in range(1, n):
            total = total + x.tland[phase, slot]
        for slot in range(n):
            value = x.tland[phase, slot]
            for face in range(FACES):
                sender = (slot - FACE_STEPS[face]) % n
                value = jnp.where(group == face + 1, x.tland[phase, sender], value)
            x.merged[slot * half : (slot + 1) * half, :] = value
        lane = lax.broadcasted_iota(jnp.int32, (ROWS, LANES), 1)
        sub = lax.broadcasted_iota(jnp.int32, (ROWS, LANES), 0)
        left = jnp.where(jnp.right_shift(lane, 3) == sub, 1.0, 0.0)
        right = jnp.where(jnp.right_shift(lane, 3) == sub + ROWS, 1.0, 0.0)
        z = self.coarse_columns(x.merged[...], left, right)
        row = total[MODES - half : MODES - half + 1, :]
        sums = [
            row_sum(jnp.where(lane == HALF + sub * ROWS + i, row, 0.0)) for i in range(4)
        ]
        return z, sums

    def exchange(self, phase, scalars, more):
        x = self.x

        def keep(at, block):
            x.y[phase, :, at] = block

        with jax.named_scope("to_face"):
            self.to_face(x.yw, 2, keep)
        with jax.named_scope("contrib"):
            ref = x.y.at[phase]
            copies = self.start_faces(phase + 1, ref)
            self.send_all(phase, self.contributions(ref, scalars(ref)))
        with jax.named_scope("f_wait"):
            for copy in copies:
                copy.wait()
        for face in range(FACES):
            span = self.span(face)
            x.a[:, span] = ref[:, span] - self.far_face(phase + 1, face)
        if more:
            with jax.named_scope("a_dof"):
                self.to_dof(x.a, 2, self.stack_vector)
            with jax.named_scope("dual_dot"):
                self.product(ROWS, x.yfresh)
        with jax.named_scope("t_wait"):
            self.wait_all(phase)
        with jax.named_scope("collect"):
            return self.collect(phase)


    def run(self, sizes_ref, neighbours_ref, counts_ref, map_ref, modes_ref, local_ref,
            goal_ref, table_ref, dual_ref, mult_out, resid_out, x):
        self.x = x
        self.me = lax.axis_index("dev")
        n, f32 = self.slots, jnp.float32
        inputs = (
            (map_ref, x.map), (counts_ref, x.counts), (neighbours_ref, x.links),
            (modes_ref, x.raw), (local_ref, x.local), (goal_ref, x.goal), (table_ref, x.table),
        )
        inputs = [
            pltpu.make_async_copy(source, target, x.in_sem.at[index])
            for index, (source, target) in enumerate(inputs)
        ]
        for copy in inputs:
            copy.start()
        barrier = pltpu.get_barrier_semaphore()
        self.others(lambda target: pl.semaphore_signal(
            barrier, inc=1, device_id=(target,), device_id_type=MESH
        ))

        with jax.named_scope("inputs"):
            for copy in inputs:
                copy.wait()
            loads = []
            for block in range(self.highs):
                at = pl.ds(block * LOW, LOW)
                copy = pltpu.make_async_copy(
                    dual_ref.at[0, at, :], x.dual.at[at, :], x.dual_sem.at[block]
                )
                copy.start()
                loads.append(copy)
        with jax.named_scope("codes"):
            columns = lax.broadcasted_iota(jnp.int32, (1, self.nmax), 1)
            x.codes[...] = jnp.where(columns < sizes_ref[0], x.map[...], -1)
            self.spread_low(x.codes, x.onehot)
            place = lax.broadcasted_iota(jnp.int32, (1, self.cap), 1)
            for face in range(FACES):
                counted = jnp.where(place < x.counts[0, face], 1.0, 0.0)
                both = jnp.where(x.links[0, face] >= 0, counted, jnp.zeros_like(counted))
                x.counted[:, self.span(face)] = counted
                x.shared[:, self.span(face)] = both
                x.weights[:, self.span(face)] = counted - 0.5 * both
            for a in range(MODES):
                x.pad[a : a + 1, :] = x.raw[a]
            x.pad[MODES : MODES + 1, :] = jnp.right_shift(columns, 8).astype(f32)
            x.pad[MODES + 1 :, :] = jnp.bitwise_and(columns, LOW - 1).astype(f32)
        with jax.named_scope("modes_face"):
            self.scatter_modes()
        with jax.named_scope("barrier_wait"):
            pl.semaphore_wait(barrier, n - 1)
            copies = self.start_faces(0, x.modes)
        with jax.named_scope("places"):
            self.own_block()
            self.spread_low(x.places, x.unhot)
        with jax.named_scope("modes_wait"):
            for copy in copies:
                copy.wait()
        with jax.named_scope("coarse_row"):
            for face in range(FACES):
                x.far[:, self.span(face)] = self.far_face(0, face)
            self.send_all(ROUNDS, self.coarse_row())
        with jax.named_scope("dual_wait"):
            for copy in loads:
                copy.wait()
        with jax.named_scope("rigid_products"):
            self.rigid_products()
        with jax.named_scope("q_wait"):
            self.wait_all(ROUNDS)
        with jax.named_scope("coarse_inverse"):
            self.coarse_inverse()

        for slot in range(n):
            x.merged[slot * ROWS // 2 : (slot + 1) * ROWS // 2, :] = x.tland[ROUNDS, slot]
        lane = lax.broadcasted_iota(jnp.int32, (ROWS, LANES), 1)
        sub = lax.broadcasted_iota(jnp.int32, (ROWS, LANES), 0)
        left = jnp.where(lane == sub + (HALF - ROWS), 1.0, 0.0)
        right = jnp.where(lane == sub + (LANES - ROWS), 1.0, 0.0)
        z = self.coarse_columns(x.merged[...], left, right)
        for face in range(FACES):
            span = self.span(face)
            x.m[:, span] = self.rigid_part(z, face)
            local = jnp.where(x.codes[:, span] >= 0, x.local[0, :, span], 0.0)
            x.yw[:, span] = local - self.rigid_product(z, span)

        z, _ = self.exchange(0, lambda ref: None, True)
        for face in range(FACES):
            span = self.span(face)
            x.w[:, span] = x.a[:, span] - self.rigid_part(z, face)
            x.yw[:, span] = x.yfresh[:, span] - self.rigid_product(z, span)

        for phase in range(1, ROUNDS):
            def scalars(ref):
                w, y = x.w[...], ref[...]
                weighted = w * x.weights[...]
                zero = jnp.zeros((ROWS, 1), f32)
                return [
                    row_sum(weighted * w),
                    row_sum(w * y),
                    row_sum(weighted * x.q[...]) if phase > 1 else zero,
                    row_sum(x.d[...] * y) if phase > 1 else zero,
                ]

            z, (rho, wa, wq, da) = self.exchange(phase, scalars, phase < ITERS)
            if phase > 1:
                beta = rho / rho_old
                curve = wa + beta * (wq + da) + beta * beta * curve
            else:
                curve = wa
            step = rho / curve
            rho_old = rho
            for face in range(FACES):
                span = self.span(face)
                applied = x.a[:, span]
                d, q, s = x.w[:, span], applied, applied - self.rigid_part(z, face)
                if phase > 1:
                    d += beta * x.d[:, span]
                    s += beta * x.s[:, span]
                x.m[:, span] += step * d
                x.w[:, span] -= step * s
                if phase < ITERS:
                    if phase > 1:
                        q += beta * x.q[:, span]
                    x.d[:, span], x.q[:, span], x.s[:, span] = d, q, s
                    ys = x.yfresh[:, span] - self.rigid_product(z, span)
                    if phase > 1:
                        ys += beta * x.ys[:, span]
                    x.ys[:, span] = ys
                    x.yw[:, span] -= step * ys

        with jax.named_scope("final"):
            for ref, out in ((x.m, mult_out), (x.w, resid_out)):
                def put(at, block, out=out):
                    out[0, :, at] = block
                self.to_dof(ref, 3, put)


class Refs:
    def __init__(self, names, refs):
        self.__dict__.update(zip(names, refs))


def per_device(
    dual_blocks, rigid_modes, dual_local, coarse_rhs, iface_sizes, neighbours, shared_counts,
    iface_map, owner,
):
    slots = lax.axis_size("dev")
    loads, nmax = dual_local.shape[1:]
    solver = Solver(slots, loads, nmax, nmax // FACES)
    scratch = solver.scratch()
    names = list(scratch)

    def kernel(*refs):
        solver.run(*refs[:11], Refs(names, refs[11:]))

    laneslot, lanemode = [-1] * solver.width, [-1] * solver.width
    for slot, at in solver.lane_of.items():
        for mode in range(MODES):
            laneslot[at + mode], lanemode[at + mode] = slot, mode
    table = jnp.array([laneslot, lanemode] + [[0] * solver.width] * 6, jnp.int32)
    vmem, smem = pl.BlockSpec(memory_space=pltpu.VMEM), pl.BlockSpec(memory_space=pltpu.SMEM)
    result = jax.ShapeDtypeStruct((1, loads, nmax), jnp.float32)
    solved = pl.pallas_call(
        kernel,
        out_shape=(pltpu.VMEM(result.shape, jnp.float32),) * 2,
        in_specs=[smem] + [pl.BlockSpec(memory_space=pltpu.HBM)] * 8,
        out_specs=(vmem, vmem),
        scratch_shapes=list(scratch.values()),
        compiler_params=pltpu.CompilerParams(
            collective_id=0, has_side_effects=True, vmem_limit_bytes=48 * 2**20
        ),
    )(iface_sizes, *[
        pltpu.with_memory_space_constraint(item, pltpu.HBM) for item in (
            neighbours, shared_counts, iface_map, rigid_modes.transpose(1, 0, 2), dual_local,
            coarse_rhs.transpose(1, 0, 2), table, dual_blocks,
        )
    ])

    def hand_over(*refs):
        copies = [pltpu.make_async_copy(refs[i], refs[2 + i], refs[4].at[i]) for i in range(2)]
        for copy in copies:
            copy.start()
        for copy in copies:
            copy.wait()

    return pl.pallas_call(
        hand_over,
        out_shape=(result, result),
        in_specs=[vmem] * 2,
        out_specs=(pl.BlockSpec(memory_space=pltpu.HBM),) * 2,
        scratch_shapes=[pltpu.SemaphoreType.DMA((2,))],
    )(*[pltpu.with_memory_space_constraint(item, pltpu.VMEM) for item in solved])


def solution(mesh):
    return jax.shard_map(
        per_device,
        mesh=mesh,
        in_specs=(
            P("dev", None, None),
            P("dev", None, None),
            P("dev", None, None),
            P("dev", None, None),
            P("dev"),
            P("dev", None),
            P("dev", None),
            P("dev", None),
            P(),
        ),
        out_specs=(P("dev", None, None), P("dev", None, None)),
        check_vma=False,
    )
```

```python
import functools

import jax
import jax.numpy as jnp
from jax import lax
from jax.experimental import pallas as pl
from jax.experimental.pallas import tpu as pltpu
from jax.sharding import PartitionSpec as P

FACES = 6
MODES = 6
ITERS = 3
ROUNDS = ITERS + 1
LANES = 128
HALF = 64
WIDE = 1536
CUT = 2048
LOW = 256
ROWS = 8
FACE_STEPS = (-1, 1, -4, 4, -16, 16)
BLOCK_STEPS = (0,) + FACE_STEPS
HIGHEST = lax.Precision.HIGHEST
MESH = pl.DeviceIdType.MESH
NN = (((1,), (0,)), ((), ()))
NT = (((1,), (1,)), ((), ()))


def coarse_order(slots):
    apart = []
    for slot in range(slots):
        if all((slot + by) % slots not in apart for by in FACE_STEPS):
            apart.append(slot)
    rest = [slot for slot in range(slots) if slot not in apart]
    first = -(-len(rest) * MODES // LANES) * LANES
    second = -(-len(apart) * MODES // LANES) * LANES
    return apart, rest, first, second


def high_dot(a, b, dims=NN):
    return lax.dot_general(
        a, b, dims, precision=HIGHEST, preferred_element_type=jnp.float32
    )


def split(value, parts):
    out = []
    for part in range(parts):
        piece = value.astype(jnp.bfloat16)
        out.append(piece)
        if part < parts - 1:
            value = value - piece.astype(jnp.float32)
    return out


def row_sum(value):
    return jnp.sum(value, axis=1, keepdims=True)


class Solver:
    def __init__(self, slots, loads, nmax, cap):
        self.slots, self.loads, self.nmax, self.cap = slots, loads, nmax, cap
        self.apart, self.rest, self.first, self.second = coarse_order(slots)
        self.width = self.first + self.second
        self.lane_of = {}
        for start, group in ((0, self.rest), (self.first, self.apart)):
            for place, slot in enumerate(group):
                self.lane_of[slot] = start + place * MODES
        self.merged = 16 % slots == -16 % slots
        self.ports = FACES - 1 if self.merged else FACES
        self.highs = nmax // LOW

    def span(self, face):
        return slice(face * self.cap, (face + 1) * self.cap)

    def scratch(self):
        f32 = jnp.float32
        n, nmax, width, ports = self.slots, self.nmax, self.width, self.ports
        vector = (ROWS, nmax)
        return dict(
            dual=pltpu.VMEM((nmax, nmax), jnp.bfloat16),
            onehot=pltpu.VMEM((LOW, nmax), jnp.bfloat16),
            stack=pltpu.VMEM((2 * ROWS * self.highs, nmax), jnp.bfloat16),
            codes=pltpu.VMEM((1, nmax), jnp.int32),
            places=pltpu.VMEM((1, nmax), jnp.int32),
            unhot=pltpu.VMEM((LOW, nmax), jnp.bfloat16),
            small=pltpu.VMEM((ROWS, LANES), f32),
            own=pltpu.VMEM((2, ROWS, LANES), f32),
            pad=pltpu.VMEM(vector, f32),
            modes=pltpu.VMEM(vector, f32),
            far=pltpu.VMEM(vector, f32),
            shared=pltpu.VMEM((1, nmax), f32),
            weights=pltpu.VMEM((1, nmax), f32),
            counted=pltpu.VMEM((1, nmax), f32),
            m=pltpu.VMEM(vector, f32),
            w=pltpu.VMEM(vector, f32),
            d=pltpu.VMEM(vector, f32),
            q=pltpu.VMEM(vector, f32),
            s=pltpu.VMEM(vector, f32),
            a=pltpu.VMEM(vector, f32),
            dofs=pltpu.VMEM(vector, f32),
            yfresh=pltpu.VMEM(vector, f32),
            yw=pltpu.VMEM(vector, f32),
            ys=pltpu.VMEM(vector, f32),
            yrigid=pltpu.VMEM((ROWS * (FACES + 1), nmax), f32),
            y=pltpu.VMEM((ROUNDS,) + vector, f32),
            zface=pltpu.VMEM((ROUNDS + 1, ROWS, self.cap), f32),
            fland=pltpu.VMEM((ROUNDS + 1, ports, ROWS, self.cap), f32),
            tsend=pltpu.VMEM((ROUNDS + 1, ROWS // 2, LANES), f32),
            tland=pltpu.VMEM((ROUNDS + 1, n, ROWS // 2, LANES), f32),
            merged=pltpu.VMEM((n * ROWS // 2, LANES), f32),
            qrows=pltpu.VMEM((n, ROWS, width), f32),
            packed=pltpu.VMEM((width, width), f32),
            dense=pltpu.VMEM((self.first, self.first), f32),
            basis=pltpu.VMEM((n * ROWS, width), f32),
            halves=pltpu.VMEM((2, n * ROWS // 2, width), f32),
            picks=pltpu.VMEM((2 * ROWS * (FACES + 1), n * ROWS // 2), f32),
            map=pltpu.VMEM((1, nmax), jnp.int32),
            raw=pltpu.VMEM((MODES, 1, nmax), f32),
            local=pltpu.VMEM((1, self.loads, nmax), f32),
            goal=pltpu.VMEM((MODES, 1, self.loads), f32),
            table=pltpu.VMEM((ROWS, width), jnp.int32),
            links=pltpu.SMEM((1, FACES), jnp.int32),
            counts=pltpu.SMEM((1, FACES), jnp.int32),
            in_sem=pltpu.SemaphoreType.DMA((7,)),
            dual_sem=pltpu.SemaphoreType.DMA((self.highs,)),
            fsend_sem=pltpu.SemaphoreType.DMA((ROUNDS + 1, ports)),
            frecv_sem=pltpu.SemaphoreType.DMA((ROUNDS + 1, ports)),
            tsend_sem=pltpu.SemaphoreType.DMA((ROUNDS + 1,)),
            trecv_sem=pltpu.SemaphoreType.DMA((ROUNDS + 1,)),
        )


    def spread_low(self, codes_ref, onehot_ref):
        def body(block, carry):
            at = pl.ds(pl.multiple_of(block * LANES, LANES), LANES)
            codes = codes_ref[:, at]
            low = jnp.where(codes < 0, -1, jnp.bitwise_and(codes, LOW - 1))
            rows = lax.broadcasted_iota(jnp.int32, (LOW, LANES), 0)
            onehot_ref[:, at] = jnp.where(rows == low, 1.0, 0.0).astype(jnp.bfloat16)
            return carry

        lax.fori_loop(0, self.nmax // LANES, body, 0)

    def scatter_modes(self):
        x, rows, parts = self.x, ROWS * self.highs, 2

        def body(block, carry):
            at = pl.ds(pl.multiple_of(block * LOW, LOW), LOW)
            high = jnp.right_shift(x.codes[:, at], 8)
            for index, piece in enumerate(split(x.pad[:, at], parts)):
                piece = piece.astype(jnp.float32)
                stacked = [jnp.where(high == h, piece, 0.0) for h in range(self.highs)]
                x.stack[index * rows : (index + 1) * rows, at] = jnp.concatenate(
                    stacked, axis=0
                ).astype(jnp.bfloat16)
            return carry

        lax.fori_loop(0, self.highs, body, 0)
        found = lax.dot_general(
            x.stack[: parts * rows], x.onehot[...], NT, preferred_element_type=jnp.float32
        )
        total = found[:rows] + found[rows:]
        sub = lax.broadcasted_iota(jnp.int32, (ROWS, LOW), 0)
        for h in range(self.highs):
            at = slice(h * LOW, (h + 1) * LOW)
            block = total[h * ROWS : (h + 1) * ROWS]
            x.modes[:, at] = jnp.where(sub < MODES, block, 0.0)
            place = block[MODES : MODES + 1] * LOW + block[MODES + 1 : MODES + 2]
            place = (place + 0.5).astype(jnp.int32)
            x.places[:, at] = jnp.where(x.counted[:, at] > 0.0, place, -1)

    def reorder(self, source, codes_ref, onehot_ref, parts, store):
        rows = ROWS * self.highs
        pieces = [split(source[:, h * LOW : (h + 1) * LOW], parts) for h in range(self.highs)]
        stacked = jnp.concatenate(
            [pieces[h][index].astype(jnp.float32) for index in range(parts)
             for h in range(self.highs)], axis=0,
        ).astype(jnp.bfloat16)
        for block in range(self.highs):
            at = slice(block * LOW, (block + 1) * LOW)
            found = jnp.dot(stacked, onehot_ref[:, at], preferred_element_type=jnp.float32)
            total = found[:rows]
            for index in range(1, parts):
                total = total + found[index * rows : (index + 1) * rows]
            high = jnp.right_shift(codes_ref[:, at], 8)
            picked = jnp.zeros((ROWS, LOW), jnp.float32)
            for h in range(self.highs):
                picked = jnp.where(high == h, total[h * ROWS : (h + 1) * ROWS], picked)
            store(at, picked)

    def to_dof(self, source, parts, store):
        self.reorder(source, self.x.codes, self.x.onehot, parts, store)

    def to_face(self, source, parts, store):
        self.reorder(source, self.x.places, self.x.unhot, parts, store)


    def others(self, act):
        def body(by, carry):
            act(lax.rem(self.me + by, self.slots))
            return carry

        lax.fori_loop(1, self.slots, body, 0)

    def face_copies(self, phase, source):
        x = self.x
        copies = []
        for port in range(self.ports):
            merged = self.merged and port == self.ports - 1
            opposite = port if merged else port ^ 1
            target = lax.rem(self.me + FACE_STEPS[port] + self.slots, self.slots)
            copies.append(pltpu.make_async_remote_copy(
                src_ref=x.zface.at[phase] if merged else source(port),
                dst_ref=x.fland.at[phase, opposite],
                send_sem=x.fsend_sem.at[phase, port],
                recv_sem=x.frecv_sem.at[phase, opposite],
                device_id=(target,),
                device_id_type=MESH,
            ))
        return copies

    def start_faces(self, phase, ref):
        x = self.x
        if self.merged:
            lower, upper = self.span(FACES - 2), self.span(FACES - 1)
            x.zface[phase] = jnp.where(x.shared[:, lower] > 0.0, ref[:, lower], ref[:, upper])
        copies = self.face_copies(phase, lambda face: ref.at[:, self.span(face)])
        for copy in copies:
            copy.start()
        return copies

    def far_face(self, phase, face):
        return self.x.fland[phase, min(face, self.ports - 1)] * self.x.shared[:, self.span(face)]

    def all_copy(self, phase, source, landing, target):
        x = self.x
        return pltpu.make_async_remote_copy(
            src_ref=source, dst_ref=landing, send_sem=x.tsend_sem.at[phase],
            recv_sem=x.trecv_sem.at[phase], device_id=(target,), device_id_type=MESH,
        )

    def send_all(self, phase, tile):
        x = self.x
        lane = lax.broadcasted_iota(jnp.int32, (ROWS // 2, LANES), 1)
        packed = jnp.where(lane < HALF, tile[: ROWS // 2], pltpu.roll(tile, HALF, 1)[ROWS // 2 :])
        x.tsend[phase] = packed
        source, landing = x.tsend.at[phase], x.tland.at[phase, self.me]
        self.others(lambda target: self.all_copy(phase, source, landing, target).start())
        x.tland[phase, self.me] = packed

    def wait_all(self, phase):
        part = self.x.tland.at[phase, pl.ds(0, self.slots - 1)]
        whole = self.all_copy(phase, part, part, lax.rem(self.me + 1, self.slots))
        whole.wait_recv()
        whole.wait_send()


    def own_inverse(self, block):
        lane = lax.broadcasted_iota(jnp.int32, (1, LANES), 1)
        sub = lax.broadcasted_iota(jnp.int32, (ROWS, 1), 0)
        for k in range(MODES):
            here = lane == k
            row, column = block[k : k + 1, :], block[:, k : k + 1]
            scale = 1.0 / block[k : k + 1, k : k + 1]
            use = row * scale
            fresh = jnp.where(here, column * scale, block - column * use)
            block = jnp.where(sub == k, jnp.where(here, -scale, use), fresh)
        return -block

    def own_block(self):
        x = self.x
        lane = lax.broadcasted_iota(jnp.int32, (1, LANES), 1)
        own = jnp.zeros((ROWS, LANES), jnp.float32)
        for b in range(MODES):
            own = jnp.where(lane == b, row_sum(x.modes[...] * x.modes[b : b + 1, :]), own)
        x.own[0], x.own[1] = own, self.own_inverse(own)
        x.small[...] = jnp.zeros((ROWS, LANES), jnp.float32)
        for a in range(MODES):
            x.small[a : a + 1, : self.loads] = x.goal[a]

    def coarse_row(self):
        x = self.x
        lane = lax.broadcasted_iota(jnp.int32, (1, LANES), 1)
        own, inverse = x.own[0], x.own[1]
        far = jnp.zeros((ROWS, LANES), jnp.float32)
        for face in range(FACES):
            span = self.span(face)
            for b in range(MODES):
                value = row_sum(x.modes[:, span] * x.far[b : b + 1, span])
                far = jnp.where(lane == (face + 1) * ROWS + b, -value, far)
        scaled = inverse
        for b in range(MODES):
            scaled += inverse[:, b : b + 1] * far[b : b + 1, :]
        apart = sum((self.me == slot).astype(jnp.int32) for slot in self.apart)
        goal = pltpu.roll(x.small[...], HALF - ROWS, 1)
        return jnp.where(apart > 0, scaled, far + own) + goal

    def spread_rows(self):
        x, n, phase = self.x, self.slots, ROUNDS
        for slot in range(n):
            packed = x.tland[phase, slot]
            tile = jnp.concatenate([packed, pltpu.roll(packed, HALF, 1)], axis=0)
            tiles = [None] * (self.width // LANES)
            for g, by in enumerate(BLOCK_STEPS):
                target = (slot + by) % n
                place = self.lane_of[target]
                for index in {place // LANES, (place + MODES - 1) // LANES}:
                    table = x.table[0:1, index * LANES : (index + 1) * LANES]
                    moved = pltpu.roll(tile, (place - g * ROWS) % LANES, 1)
                    part = jnp.where(table == target, moved, 0.0)
                    tiles[index] = part if tiles[index] is None else tiles[index] + part
            for index, part in enumerate(tiles):
                if part is None:
                    part = jnp.zeros((ROWS, LANES), jnp.float32)
                x.qrows[slot, :, index * LANES : (index + 1) * LANES] = part

    def eliminate(self):
        out = self.x.dense
        lane = lax.broadcasted_iota(jnp.int32, (1, self.first), 1)
        modes = range(MODES)

        def body(step, carry):
            k = step * MODES
            at = [lane == k + a for a in modes]
            rows = [out[pl.ds(k + a, 1), :] for a in modes]
            block = [[None] * MODES for a in modes]
            for a in modes:
                for b in range(a, MODES):
                    block[a][b] = row_sum(jnp.where(at[b], rows[a], 0.0))
                    block[b][a] = block[a][b]
            for c in modes:
                scale = 1.0 / block[c][c]
                column = [block[a][c] for a in modes]
                use = [column[a] * scale for a in modes]
                for a in modes:
                    for b in range(a, MODES):
                        if a == c and b == c:
                            fresh = -scale
                        elif b == c:
                            fresh = use[a]
                        elif a == c:
                            fresh = use[b]
                        else:
                            fresh = block[a][b] - column[a] * use[b]
                        block[a][b] = block[b][a] = fresh
            uses = []
            for a in modes:
                use = -block[a][0] * rows[0]
                for b in range(1, MODES):
                    use -= block[a][b] * rows[b]
                for b in modes:
                    use = jnp.where(at[b], block[a][b], use)
                uses.append(use)
            whole = out[...]
            fresh = jnp.where((lane >= k) & (lane < k + MODES), 0.0, whole)
            for a in modes:
                fresh -= row_sum(jnp.where(at[a], whole, 0.0)) * uses[a]
            out[...] = fresh
            for a in modes:
                out[pl.ds(k + a, 1), :] = uses[a]
            return carry

        lax.fori_loop(0, len(self.rest), body, 0)

    def coarse_inverse(self):
        x, n, first, half = self.x, self.slots, self.first, ROWS // 2
        self.spread_rows()
        x.packed[...] = jnp.zeros(x.packed.shape, jnp.float32)
        for slot in range(n):
            at = self.lane_of[slot]
            x.packed[at : at + MODES, :] = x.qrows[slot, :MODES, :]
        x.dense[...] = x.packed[:first, :first] - high_dot(
            x.packed[:first, first:], x.packed[first:, :first]
        )
        with jax.named_scope("eliminate"):
            self.eliminate()
        laneslot, lanemode = x.table[0:1, :], x.table[1:2, :]
        lane = lax.broadcasted_iota(jnp.int32, (1, self.width), 1)
        sub = lax.broadcasted_iota(jnp.int32, (ROWS, 1), 0)
        for slot in range(n):
            unit = jnp.where((laneslot == slot) & (lanemode == sub), 1.0, 0.0)
            if slot in self.apart:
                unit -= jnp.where((lane < first) & (sub < MODES), x.qrows[slot], 0.0)
            x.basis[slot * ROWS : (slot + 1) * ROWS, :] = unit
            x.halves[0, slot * half : (slot + 1) * half, :] = unit[:half]
            x.halves[1, slot * half : (slot + 1) * half, :] = unit[half:]
        chosen = jnp.concatenate([
            x.basis[pl.ds(pl.multiple_of(lax.rem(self.me + by + n, n) * ROWS, ROWS), ROWS), :]
            for by in BLOCK_STEPS
        ], axis=0)
        solved = jnp.concatenate([
            -high_dot(chosen[:, :first], x.dense[...]),
            high_dot(chosen[:, first:], x.packed[first:, first:]),
        ], axis=1)
        rows = chosen.shape[0]
        x.picks[:rows] = high_dot(solved, x.halves[0], NT)
        x.picks[rows:] = high_dot(solved, x.halves[1], NT)

    def coarse_columns(self, values, left, right):
        found = high_dot(self.x.picks[...], values)
        rows = ROWS * (FACES + 1)
        return [
            [row_sum(found[at : at + 1] * left + found[rows + at : rows + at + 1] * right)
             for at in range(g * ROWS, g * ROWS + MODES)]
            for g in range(FACES + 1)
        ]

    def rigid_part(self, z, face):
        x, span = self.x, self.span(face)
        total = jnp.zeros((ROWS, self.cap), jnp.float32)
        for a in range(MODES):
            total += z[0][a] * x.modes[a : a + 1, span]
            total -= z[face + 1][a] * x.far[a : a + 1, span]
        return total


    def rigid_product(self, z, at):
        total = z[0][0] * self.x.yrigid[0:1, at]
        for g in range(FACES + 1):
            for a in range(MODES):
                if g or a:
                    total += z[g][a] * self.x.yrigid[g * ROWS + a : g * ROWS + a + 1, at]
        return total

    def product(self, rows, out, at):
        x = self.x
        both = jnp.dot(
            x.stack[: 2 * rows, :], x.dual[:, at], preferred_element_type=jnp.float32
        )
        out[:, at] = both[:rows] + both[rows:]

    def stack_vector(self, at, block):
        parts = [piece.astype(jnp.float32) for piece in split(block, 2)]
        self.x.stack[: 2 * ROWS, at] = jnp.concatenate(parts, axis=0).astype(jnp.bfloat16)

    def rigid_products(self):
        x = self.x

        def keep(at, block):
            x.dofs[:, at] = block

        self.to_dof(x.far, 2, keep)
        sub = lax.broadcasted_iota(jnp.int32, (ROWS, LOW), 0)
        for block in range(self.highs):
            at = slice(block * LOW, (block + 1) * LOW)
            codes = x.codes[:, at]
            own = jnp.where((codes >= 0) & (sub < MODES), x.pad[:, at], 0.0)
            own = [piece.astype(jnp.float32) for piece in split(own, 2)]
            far = [piece.astype(jnp.float32) for piece in split(-x.dofs[:, at], 2)]
            rows = []
            for index in range(2):
                rows.append(own[index])
                for face in range(FACES):
                    here = (codes >= face * self.cap) & (codes < (face + 1) * self.cap)
                    rows.append(jnp.where(here, far[index], 0.0))
            x.stack[: len(rows) * ROWS, at] = jnp.concatenate(rows, axis=0).astype(jnp.bfloat16)

        def body(block, carry):
            at = pl.ds(pl.multiple_of(block * WIDE, WIDE), WIDE)
            self.product(ROWS * (FACES + 1), x.yrigid, at)
            return carry

        lax.fori_loop(0, self.nmax // WIDE, body, 0)

    def contributions(self, ref, scalars):
        x = self.x
        lane = lax.broadcasted_iota(jnp.int32, (ROWS, LANES), 1)
        sub = lax.broadcasted_iota(jnp.int32, (ROWS, LANES), 0)
        out = jnp.zeros((ROWS, LANES), jnp.float32)
        for load in range(self.loads):
            own = jnp.zeros((ROWS, self.cap), jnp.float32)
            for face in range(FACES):
                span = self.span(face)
                row = ref[load : load + 1, span]
                own += x.modes[:, span] * row
                other = row_sum(x.far[:, span] * row)
                out = jnp.where(lane == load * ROWS + face + 1, -other, out)
            out = jnp.where(lane == load * ROWS, row_sum(own), out)
        if scalars:
            spread = jnp.zeros((ROWS, LANES), jnp.float32)
            for index, value in enumerate(scalars):
                spread = jnp.where(lane == sub * ROWS + index, value, spread)
            out = jnp.where(sub == MODES, jnp.sum(spread, axis=0, keepdims=True), out)
        return out

    def collect(self, phase):
        x, n, half = self.x, self.slots, ROWS // 2
        group = jnp.bitwise_and(lax.broadcasted_iota(jnp.int32, (half, LANES), 1), ROWS - 1)
        total = x.tland[phase, 0]
        for slot in range(1, n):
            total = total + x.tland[phase, slot]
        for slot in range(n):
            value = x.tland[phase, slot]
            for face in range(FACES):
                sender = (slot - FACE_STEPS[face]) % n
                value = jnp.where(group == face + 1, x.tland[phase, sender], value)
            x.merged[slot * half : (slot + 1) * half, :] = value
        lane = lax.broadcasted_iota(jnp.int32, (ROWS, LANES), 1)
        sub = lax.broadcasted_iota(jnp.int32, (ROWS, LANES), 0)
        left = jnp.where(jnp.right_shift(lane, 3) == sub, 1.0, 0.0)
        right = jnp.where(jnp.right_shift(lane, 3) == sub + ROWS, 1.0, 0.0)
        z = self.coarse_columns(x.merged[...], left, right)
        row = total[MODES - half : MODES - half + 1, :]
        sums = [
            row_sum(jnp.where(lane == HALF + sub * ROWS + i, row, 0.0)) for i in range(4)
        ]
        return z, sums

    def exchange(self, phase, scalars, more):
        x = self.x

        def keep(at, block):
            x.y[phase, :, at] = block

        with jax.named_scope("to_face"):
            self.to_face(x.yw, 2, keep)
        ref = x.y.at[phase]
        if more:
            copies = self.start_faces(phase + 1, ref)
            self.send_all(phase, self.contributions(ref, scalars(ref)))
        else:
            self.send_all(phase, self.contributions(ref, scalars(ref)))
            copies = self.start_faces(phase + 1, ref)
        with jax.named_scope("f_wait"):
            for copy in copies:
                copy.wait()
        for face in range(FACES):
            span = self.span(face)
            x.a[:, span] = ref[:, span] - self.far_face(phase + 1, face)
        if more:
            with jax.named_scope("a_dof"):
                self.to_dof(x.a, 2, self.stack_vector)
            with jax.named_scope("dual_dot"):
                self.product(ROWS, x.yfresh, slice(0, CUT))
        with jax.named_scope("t_wait"):
            self.wait_all(phase)
        with jax.named_scope("collect"):
            found = self.collect(phase)
            if more:
                self.product(ROWS, x.yfresh, slice(CUT, self.nmax))
            return found


    def run(self, sizes_ref, neighbours_ref, counts_ref, map_ref, modes_ref, local_ref,
            goal_ref, table_ref, dual_ref, mult_out, resid_out, x):
        self.x = x
        self.me = lax.axis_index("dev")
        n, f32 = self.slots, jnp.float32
        inputs = (
            (map_ref, x.map), (counts_ref, x.counts), (neighbours_ref, x.links),
            (modes_ref, x.raw), (local_ref, x.local), (goal_ref, x.goal), (table_ref, x.table),
        )
        inputs = [
            pltpu.make_async_copy(source, target, x.in_sem.at[index])
            for index, (source, target) in enumerate(inputs)
        ]
        for copy in inputs:
            copy.start()
        barrier = pltpu.get_barrier_semaphore()
        self.others(lambda target: pl.semaphore_signal(
            barrier, inc=1, device_id=(target,), device_id_type=MESH
        ))

        with jax.named_scope("inputs"):
            for copy in inputs:
                copy.wait()
            loads = []
            for block in range(self.highs):
                at = pl.ds(block * LOW, LOW)
                copy = pltpu.make_async_copy(
                    dual_ref.at[0, at, :], x.dual.at[at, :], x.dual_sem.at[block]
                )
                copy.start()
                loads.append(copy)
        with jax.named_scope("codes"):
            columns = lax.broadcasted_iota(jnp.int32, (1, self.nmax), 1)
            x.codes[...] = jnp.where(columns < sizes_ref[0], x.map[...], -1)
            self.spread_low(x.codes, x.onehot)
            place = lax.broadcasted_iota(jnp.int32, (1, self.cap), 1)
            for face in range(FACES):
                counted = jnp.where(place < x.counts[0, face], 1.0, 0.0)
                both = jnp.where(x.links[0, face] >= 0, counted, jnp.zeros_like(counted))
                x.counted[:, self.span(face)] = counted
                x.shared[:, self.span(face)] = both
                x.weights[:, self.span(face)] = counted - 0.5 * both
            for a in range(MODES):
                x.pad[a : a + 1, :] = x.raw[a]
            x.pad[MODES : MODES + 1, :] = jnp.right_shift(columns, 8).astype(f32)
            x.pad[MODES + 1 :, :] = jnp.bitwise_and(columns, LOW - 1).astype(f32)
        with jax.named_scope("modes_face"):
            self.scatter_modes()
        with jax.named_scope("barrier_wait"):
            pl.semaphore_wait(barrier, n - 1)
            copies = self.start_faces(0, x.modes)
        with jax.named_scope("places"):
            self.own_block()
            self.spread_low(x.places, x.unhot)
        with jax.named_scope("modes_wait"):
            for copy in copies:
                copy.wait()
        with jax.named_scope("coarse_row"):
            for face in range(FACES):
                x.far[:, self.span(face)] = self.far_face(0, face)
            self.send_all(ROUNDS, self.coarse_row())
        with jax.named_scope("dual_wait"):
            for copy in loads:
                copy.wait()
        with jax.named_scope("rigid_products"):
            self.rigid_products()
        with jax.named_scope("q_wait"):
            self.wait_all(ROUNDS)
        with jax.named_scope("coarse_inverse"):
            self.coarse_inverse()

        for slot in range(n):
            x.merged[slot * ROWS // 2 : (slot + 1) * ROWS // 2, :] = x.tland[ROUNDS, slot]
        lane = lax.broadcasted_iota(jnp.int32, (ROWS, LANES), 1)
        sub = lax.broadcasted_iota(jnp.int32, (ROWS, LANES), 0)
        left = jnp.where(lane == sub + (HALF - ROWS), 1.0, 0.0)
        right = jnp.where(lane == sub + (LANES - ROWS), 1.0, 0.0)
        z = self.coarse_columns(x.merged[...], left, right)
        for face in range(FACES):
            span = self.span(face)
            x.m[:, span] = self.rigid_part(z, face)
            local = jnp.where(x.codes[:, span] >= 0, x.local[0, :, span], 0.0)
            x.yw[:, span] = local - self.rigid_product(z, span)

        z, _ = self.exchange(0, lambda ref: None, True)
        for face in range(FACES):
            span = self.span(face)
            x.w[:, span] = x.a[:, span] - self.rigid_part(z, face)
        for face in range(FACES):
            span = self.span(face)
            x.yw[:, span] = x.yfresh[:, span] - self.rigid_product(z, span)

        for phase in range(1, ROUNDS):
            def scalars(ref):
                w, y = x.w[...], ref[...]
                weighted = w * x.weights[...]
                zero = jnp.zeros((ROWS, 1), f32)
                return [
                    row_sum(weighted * w),
                    row_sum(w * y),
                    row_sum(weighted * x.q[...]) if phase > 1 else zero,
                    row_sum(x.d[...] * y) if phase > 1 else zero,
                ]

            z, (rho, wa, wq, da) = self.exchange(phase, scalars, phase < ITERS)
            if phase > 1:
                beta = rho / rho_old
                curve = wa + beta * (wq + da) + beta * beta * curve
            else:
                curve = wa
            step = rho / curve
            rho_old = rho
            for face in range(FACES):
                span = self.span(face)
                applied = x.a[:, span]
                d, q, s = x.w[:, span], applied, applied - self.rigid_part(z, face)
                if phase > 1:
                    d += beta * x.d[:, span]
                    s += beta * x.s[:, span]
                x.m[:, span] += step * d
                x.w[:, span] -= step * s
                if phase < ITERS:
                    if phase > 1:
                        q += beta * x.q[:, span]
                    x.d[:, span], x.q[:, span], x.s[:, span] = d, q, s
            if phase < ITERS:
                for face in range(FACES):
                    span = self.span(face)
                    ys = x.yfresh[:, span] - self.rigid_product(z, span)
                    if phase > 1:
                        ys += beta * x.ys[:, span]
                    x.ys[:, span] = ys
                    x.yw[:, span] -= step * ys

        with jax.named_scope("final"):
            for ref, out in ((x.m, mult_out), (x.w, resid_out)):
                def put(at, block, out=out):
                    out[0, :, at] = block
                self.to_dof(ref, 2, put)


class Refs:
    def __init__(self, names, refs):
        self.__dict__.update(zip(names, refs))


def per_device(
    dual_blocks, rigid_modes, dual_local, coarse_rhs, iface_sizes, neighbours, shared_counts,
    iface_map, owner,
):
    slots = lax.axis_size("dev")
    loads, nmax = dual_local.shape[1:]
    solver = Solver(slots, loads, nmax, nmax // FACES)
    scratch = solver.scratch()
    names = list(scratch)

    def kernel(*refs):
        solver.run(*refs[:11], Refs(names, refs[11:]))

    laneslot, lanemode = [-1] * solver.width, [-1] * solver.width
    for slot, at in solver.lane_of.items():
        for mode in range(MODES):
            laneslot[at + mode], lanemode[at + mode] = slot, mode
    table = jnp.array([laneslot, lanemode] + [[0] * solver.width] * 6, jnp.int32)
    vmem, smem = pl.BlockSpec(memory_space=pltpu.VMEM), pl.BlockSpec(memory_space=pltpu.SMEM)
    result = jax.ShapeDtypeStruct((1, loads, nmax), jnp.float32)
    solved = pl.pallas_call(
        kernel,
        out_shape=(pltpu.VMEM(result.shape, jnp.float32),) * 2,
        in_specs=[smem] + [pl.BlockSpec(memory_space=pltpu.HBM)] * 8,
        out_specs=(vmem, vmem),
        scratch_shapes=list(scratch.values()),
        compiler_params=pltpu.CompilerParams(
            collective_id=0, has_side_effects=True, vmem_limit_bytes=48 * 2**20
        ),
    )(iface_sizes, *[
        pltpu.with_memory_space_constraint(item, pltpu.HBM) for item in (
            neighbours, shared_counts, iface_map, rigid_modes.transpose(1, 0, 2), dual_local,
            coarse_rhs.transpose(1, 0, 2), table, dual_blocks,
        )
    ])

    def hand_over(*refs):
        copies = [pltpu.make_async_copy(refs[i], refs[2 + i], refs[4].at[i]) for i in range(2)]
        for copy in copies:
            copy.start()
        for copy in copies:
            copy.wait()

    return pl.pallas_call(
        hand_over,
        out_shape=(result, result),
        in_specs=[vmem] * 2,
        out_specs=(pl.BlockSpec(memory_space=pltpu.HBM),) * 2,
        scratch_shapes=[pltpu.SemaphoreType.DMA((2,))],
    )(*[pltpu.with_memory_space_constraint(item, pltpu.VMEM) for item in solved])


def solution(mesh):
    return jax.shard_map(
        per_device,
        mesh=mesh,
        in_specs=(
            P("dev", None, None),
            P("dev", None, None),
            P("dev", None, None),
            P("dev", None, None),
            P("dev"),
            P("dev", None),
            P("dev", None),
            P("dev", None),
            P(),
        ),
        out_specs=(P("dev", None, None), P("dev", None, None)),
        check_vma=False,
    )
```
